512 devices in a mesh: seq: 64 (over x, z, core), res: 8 (over y).
Axes of the slice: x: 4, y: 8, z: 8, core: 2. Of those that a mesh axis runs over, the one named last changes fastest.
Arguments:
- alignment_rows: bfloat16 [4096, 64, 64], P('seq', 'res'), may hold values from -6 to 6
- pair_features: bfloat16 [64, 64, 128], P('res', 'seq'), may hold values from -6 to 6
- sequence_block_count: int32 [64], P('seq'), may hold values from 16 to 64
- cluster_member_count: int32 [4096], P('seq'), may hold values from 1 to 16
- residue_present_mask: int32 [64], replicated, may hold values 0 or 1
- attention_in_weight: bfloat16 [64, 256], replicated, may hold values from -0.75 to 0.75
- attention_out_weight: bfloat16 [64, 64], replicated, may hold values from -4 to 4
- pair_bias_weight: float32 [128, 8], replicated, may hold values from -48 to 48
- outer_factor_weight: bfloat16 [64, 64], replicated, may hold values from -0.75 to 0.75
- outer_output_weight: float32 [1024, 128], replicated, may hold values from -4 to 4
- outer_product_bias: float32 [128], replicated, may hold values from -3 to 3
Outputs:
- row_attention_update: bfloat16 [4096, 64, 64], P('seq', 'res')
- pair_update: bfloat16 [64, 64, 128], P('seq', 'res')
The draws below stay inside these ranges and needn't reach their ends.
All inputs are finite; a program needn't handle non-finite values.
Results may differ from the reference program's by a relative error of at most 0.0081.
Values may be sent and summed in bfloat16 or wider, within the bound.
A program may use at most 64 MiB of HBM per device.

```python
import math
import jax
import jax.numpy as jnp
from jax import lax

CHANNEL_COUNT = 64
CP = 128
CO = 32
HEADS = 8
HEAD_DIM = 8
SLOT_DEV = 64
RES_DEV = 8
SLOT_TOTAL = 4096
RESIDUE_TOTAL = 64
N_SEQ = 64
N_RES = 8


def draw_pair_bias_weight(key, part):
    values = jax.random.normal(key, (CP, HEADS), jnp.float32) * (2.0 / math.sqrt(CP))
    return jnp.clip(values, -48.0, 48.0)


def plant(values, key, low, top_value):
    index_at = [jax.random.randint(jax.random.fold_in(key, axis), (), 0, length) for axis, length in enumerate(values.shape)]
    widest = values.shape.index(max(values.shape))
    neighbour = index_at[:widest] + [(index_at[widest] + 1) % values.shape[widest]] + index_at[widest + 1:]
    return values.at[tuple(index_at)].set(low).at[tuple(neighbour)].set(top_value)


def level_of(key, shape, split, low, high):
    level = 1.0
    for position, blocks in split:
        steps = jax.random.uniform(jax.random.fold_in(jax.random.fold_in(key, 6), position), (blocks,), jnp.float32, low / len(split), high / len(split))
        level = level * jnp.repeat(jnp.exp(steps), shape[position] // blocks).reshape((-1,) + (1,) * (len(shape) - 1 - position))
    return level


def centred(rng, dims, scale, reach, split=(), kind=jnp.bfloat16):
    drawn = jax.random.normal(rng, dims, jnp.float32) * scale
    if len(split) > 0:
        drawn = level_of(rng, dims, split, -0.22, 0.18) * drawn
    return jnp.clip(drawn, min=-reach, max=reach).astype(kind)


def setup_inputs(seed: int = 0) -> dict:
    arg_keys = jax.random.split(jax.random.key(seed), 12)
    return {
        "alignment_rows": centred(arg_keys[0], (SLOT_TOTAL, RESIDUE_TOTAL, CHANNEL_COUNT), 1.0, 6.0, ((0, 64), (1, 8))),
        "pair_features": centred(arg_keys[1], (RESIDUE_TOTAL, RESIDUE_TOTAL, CP), 1.0, 6.0, ((0, 8), (1, 64))),
        "sequence_block_count": plant(jax.random.randint(arg_keys[2], (N_SEQ,), SLOT_DEV // 4, SLOT_DEV + 1), jax.random.fold_in(arg_keys[2], 1), SLOT_DEV // 4, SLOT_DEV).astype(jnp.int32),
        "cluster_member_count": plant(jax.random.randint(arg_keys[3], (SLOT_TOTAL,), 1, 17), jax.random.fold_in(arg_keys[3], 1), 1, 16).astype(jnp.int32),
        "residue_present_mask": plant((jax.random.randint(arg_keys[4], (RESIDUE_TOTAL,), 0, 8) < 7).astype(jnp.int32), jax.random.fold_in(arg_keys[4], 1), 0, 1),
        "attention_in_weight": centred(arg_keys[5], (CHANNEL_COUNT, 4 * CHANNEL_COUNT), CHANNEL_COUNT ** -0.5, 0.75),
        "attention_out_weight": centred(arg_keys[6], (CHANNEL_COUNT, CHANNEL_COUNT), 1.0, 4.0),
        "pair_bias_weight": draw_pair_bias_weight(jax.random.fold_in(arg_keys[11], 71), 0),
        "outer_factor_weight": centred(arg_keys[8], (CHANNEL_COUNT, 2 * CO), CHANNEL_COUNT ** -0.5, 0.75),
        "outer_output_weight": centred(arg_keys[9], (CO * CO, CP), 1.0, 4.0, (), jnp.float32),
        "outer_product_bias": centred(arg_keys[10], (CP,), 0.5, 3.0, (), jnp.float32),
    }


def apply_layer_norm(values):
    centre = lax.optimization_barrier(jnp.mean(values, axis=-1, keepdims=True))
    spread = lax.optimization_barrier(jnp.mean(jnp.square(values - centre), axis=-1, keepdims=True))
    return (values - centre) * lax.rsqrt(spread + 1e-05)

def attend_block(pieces, full_bias):
    query_rows, key_value_pairs, gate_activation = pieces
    slot_count, n_query, channel_width = query_rows.shape
    head_count = full_bias.shape[0]
    head_dim = channel_width // head_count
    n_keys = key_value_pairs.shape[1]
    query_heads = query_rows.astype(jnp.float32).reshape(slot_count, n_query, head_count, head_dim)
    key_heads = key_value_pairs[..., :channel_width].astype(jnp.float32).reshape(slot_count, n_keys, head_count, head_dim)
    value_heads = key_value_pairs[..., channel_width:].astype(jnp.float32).reshape(slot_count, n_keys, head_count, head_dim)
    scores = jnp.einsum('bihd,bjhd->bhij', query_heads, key_heads, precision=lax.Precision.HIGHEST) + full_bias[None]
    row_max = lax.optimization_barrier(jnp.max(scores, axis=-1, keepdims=True))
    expo = jnp.exp(scores - row_max)
    probs = (expo / lax.optimization_barrier(jnp.sum(expo, axis=-1, keepdims=True))).astype(jnp.bfloat16)
    context = jnp.einsum('bhij,bjhd->bihd', probs.astype(jnp.float32), value_heads, precision=lax.Precision.HIGHEST)
    return (gate_activation * context.reshape(slot_count, n_query, channel_width)).astype(jnp.bfloat16)

def reference(alignment_rows, pair_features, sequence_block_count, cluster_member_count, residue_present_mask, attention_in_weight, attention_out_weight, pair_bias_weight, outer_factor_weight, outer_output_weight, outer_product_bias):
    total_count = SLOT_DEV * N_SEQ
    block_length = RES_DEV * N_RES
    slot_ids = jnp.arange(total_count, dtype=jnp.int32)
    usable = (slot_ids % SLOT_DEV < sequence_block_count[slot_ids // SLOT_DEV]).astype(jnp.float32)
    seq_weight = cluster_member_count.astype(jnp.float32) * usable
    weight_sum = jnp.sum(seq_weight)
    key_mask = jnp.where(residue_present_mask == 1, 0.0, -1000000.0).astype(jnp.float32)
    pair_norm = apply_layer_norm(pair_features.astype(jnp.float32))
    pair_bias = jnp.einsum('ijp,ph->hij', pair_norm, pair_bias_weight, precision=lax.Precision.HIGHEST) + key_mask[None, None, :]
    normed_alignment = apply_layer_norm(alignment_rows.astype(jnp.float32)).astype(jnp.bfloat16)
    projected_rows = jnp.dot(normed_alignment.reshape(-1, CHANNEL_COUNT), attention_in_weight, preferred_element_type=jnp.float32).reshape(total_count, block_length, 4 * CHANNEL_COUNT)
    query_rows = (projected_rows[..., :CHANNEL_COUNT] * (1.0 / math.sqrt(HEAD_DIM))).astype(jnp.bfloat16)
    key_value_pairs = projected_rows[..., CHANNEL_COUNT:3 * CHANNEL_COUNT].astype(jnp.bfloat16)
    gate_activation = jax.nn.sigmoid(projected_rows[..., 3 * CHANNEL_COUNT:])
    gated = lax.map(lambda pieces: attend_block(pieces, pair_bias), (query_rows.reshape(N_SEQ, SLOT_DEV, block_length, CHANNEL_COUNT), key_value_pairs.reshape(N_SEQ, SLOT_DEV, block_length, 2 * CHANNEL_COUNT), gate_activation.reshape(N_SEQ, SLOT_DEV, block_length, CHANNEL_COUNT)))
    update = jnp.dot(gated.reshape(-1, CHANNEL_COUNT), attention_out_weight, preferred_element_type=jnp.float32).astype(jnp.bfloat16)
    row_attention_update = update.reshape(total_count, block_length, CHANNEL_COUNT) * usable.astype(jnp.bfloat16)[:, None, None]
    updated_alignment = alignment_rows.astype(jnp.float32) + row_attention_update.astype(jnp.float32)
    outer_input_norm = apply_layer_norm(updated_alignment).astype(jnp.bfloat16)
    factors = jnp.dot(outer_input_norm.reshape(-1, CHANNEL_COUNT), outer_factor_weight, preferred_element_type=jnp.float32).reshape(total_count, block_length, 2 * CO)
    res_keep = residue_present_mask.astype(jnp.float32)[None, :, None]
    left_proj = (factors[..., :CO] * res_keep).astype(jnp.bfloat16)
    right_proj = (factors[..., CO:] * res_keep * seq_weight[:, None, None]).astype(jnp.bfloat16)
    outer = lax.dot_general(left_proj.reshape(total_count, block_length * CO).astype(jnp.float32), right_proj.reshape(total_count, block_length * CO).astype(jnp.float32), (((0,), (0,)), ((), ())), precision=lax.Precision.HIGHEST)
    outer = outer.reshape(block_length, CO, block_length, CO)
    projected = jnp.einsum('icjd,cdp->ijp', outer, outer_output_weight.reshape(CO, CO, CP), precision=lax.Precision.HIGHEST)
    pair_update = (projected / weight_sum + outer_product_bias).astype(jnp.bfloat16)
    return (row_attention_update, pair_update)
```

```python
import functools
import math

import jax
import jax.numpy as jnp
from jax import lax
from jax.experimental import pallas as pl
from jax.experimental.pallas import tpu as pltpu
from jax.sharding import PartitionSpec as P

F32 = jnp.float32
BF16 = jnp.bfloat16
MESH = pl.DeviceIdType.MESH
HI = lax.Precision.HIGHEST
N_SEQ, N_RES = 64, 8
NX, NZ, NC = 4, 8, 2


def iota(shape, dim):
    return lax.broadcasted_iota(jnp.int32, shape, dim)


def where(cond, a, b):
    return jnp.where(cond, a, b)


def mm(a, b):
    return jnp.dot(a, b, preferred_element_type=F32)


def mm_nt(a, b, precision=None):
    dims = (((1,), (1,)), ((), ()))
    return lax.dot_general(a, b, dims, precision=precision, preferred_element_type=F32)


def mm_tn(a, b):
    return mm(a.T, b)


def norm_rows(v, axis):
    centre = jnp.mean(v, axis=axis, keepdims=True)
    spread = jnp.mean(jnp.square(v - centre), axis=axis, keepdims=True)
    return (v - centre) * lax.rsqrt(spread + 1e-05)


def wait_bytes(ref, sem):
    pltpu.make_async_copy(ref, ref, sem).wait()


def kernel(
    x_ref, pf_ref, cnt_ref, cmc_ref, mask_ref, win_ref, wout_ref, wb_ref, wf_ref, ow_ref, ob_ref,
    upd_ref, pair_ref,
    xs, xr, bs, br, b2s, b2r, ls, lr, rs, rr, us, ur, ps, pr, w1s, w1r, w2s, w2r,
    tt, w4, bias2, rows,
    x_ss, x_rs, b_ss, b_rs, b2_ss, b2_rs, l_ss, l_rs, r_ss, r_rs, u_ss, u_rs, p_ss, p_rs,
    w1_ss, w1_rs, w2_ss, w2_rs,
):
    b = lax.axis_index("seq")
    r = lax.axis_index("res")
    bx = b // (NZ * NC)
    bz = (b // NC) % NZ
    bc = b % NC

    def res_peer(k):
        return (r + k) % N_RES

    def seq_peer(k):
        kc = 1 - k % 2
        tz = (k // 2) % NZ
        tx = k // (NZ * NC)
        kz = NZ // 2 + ((tz + 1) // 2) * (1 - 2 * (tz % 2))
        kx = NX // 2 + ((tx + 1) // 2) * (1 - 2 * (tx % 2))
        return ((bx + kx) % NX) * (NZ * NC) + ((bz + kz) % NZ) * NC + (bc + kc) % NC

    barrier = pltpu.get_barrier_semaphore()

    def greet(k, carry):
        pl.semaphore_signal(barrier, inc=1, device_id=(seq_peer(k), r), device_id_type=MESH)
        return carry

    lax.fori_loop(0, N_SEQ - 1, greet, 0)
    for k in range(1, N_RES):
        pl.semaphore_signal(barrier, inc=1, device_id=(b, res_peer(k)), device_id_type=MESH)

    pn = norm_rows(pf_ref[...].astype(F32), -1)
    pn = jnp.concatenate([pn] * 16, axis=0)
    pn = where((iota((128, 128), 0) // 8) % 8 == r, pn, 0.0)
    full = mm_nt(wb_ref[...].T, pn, HI)
    low = iota((4, 128), 1) < 64
    tile = where(low, full[0:4], full[4:8])
    bs[...] = tile
    br[pl.ds(r, 1)] = tile[None]

    flat = x_ref[...].astype(F32).reshape(512, 64).astype(BF16)
    dup = where(iota((64, 128), 1) % 64 == iota((64, 128), 0), 1.0, 0.0).astype(BF16)
    wide = mm(flat, dup).reshape(32, 2, 8, 128)
    pairs = where(iota((32, 8, 128), 2) < 64, wide[:, 0], wide[:, 1])
    xs[...] = pairs.reshape(8, 4, 8, 128).astype(BF16)
    xr[pl.ds(r, 1)] = xs[pl.ds(r, 1)]

    count = cnt_ref[0]
    total = jnp.float32(0.0)
    for s in range(64):
        total = total + where(s < count, cmc_ref[s], 0).astype(F32)
    w1s[...] = jnp.full((8, 128), 1.0, F32) * total
    w1r[pl.ds(bz, 1)] = w1s[...][None]
    use = []
    weight = []
    for s in range(8):
        slot = r * 8 + s
        on = where(slot < count, 1.0, 0.0)
        use.append(on)
        weight.append(cmc_ref[slot].astype(F32) * on)

    row = jnp.broadcast_to(mask_ref[...].astype(F32), (64, 64))
    keep = jnp.sum(where(iota((64, 64), 0) == iota((64, 64), 1), row, 0.0), axis=1, keepdims=True)
    key_mask = where(keep == 1.0, 0.0, -1000000.0)

    lane_u = iota((64, 128), 1) // 32
    parts = []
    for sp in range(2):
        part = jnp.zeros((64, 128), F32)
        for u in range(4):
            part = where(lane_u == u, weight[2 * u + sp], part)
        parts.append(part * keep)
    scale_r = jnp.concatenate(parts, axis=0)

    winT = win_ref[...].astype(F32).T.astype(BF16)
    woutT = wout_ref[...].astype(F32).T.astype(BF16)
    wout2 = mm(wout_ref[...], dup).astype(BF16)
    e_left = where(iota((64, 256), 0) == iota((64, 256), 1) // 8, 1.0, 0.0).astype(BF16)
    e_right = where(iota((64, 128), 0) == 32 + iota((64, 128), 1) % 32, 1.0, 0.0).astype(BF16)
    wl = mm(wf_ref[...], e_left).astype(BF16)
    wr = mm(wf_ref[...], e_right).astype(BF16)
    for c in range(32):
        block = ow_ref[pl.ds(c * 32, 32), :].astype(BF16)
        for q in range(4):
            w4[c // 2, pl.ds(q * 32, 32), pl.ds((c % 2) * 128, 128)] = block

    pl.semaphore_wait(barrier, N_SEQ - 1 + N_RES - 1)

    def send(src, dst, ss, rsem, dev):
        pltpu.make_async_remote_copy(
            src_ref=src, dst_ref=dst, send_sem=ss, recv_sem=rsem, device_id=dev, device_id_type=MESH
        ).start()

    far_first = (4, 3, 5, 2, 6, 1, 7)
    for k in far_first:
        send(bs, br.at[r], b_ss, b_rs, (b, res_peer(k)))
    for k in far_first:
        p = res_peer(k)
        send(xs.at[p], xr.at[r], x_ss, x_rs, (b, p))
    for k in far_first:
        peer = bx * (NZ * NC) + ((bz + k) % NZ) * NC + bc
        send(w1s, w1r.at[bz], w1_ss, w1_rs, (peer, r))

    wait_bytes(br.at[pl.ds(0, 7)], b_rs)
    tile2 = jnp.sum(br[...], axis=0)
    b2s[...] = tile2
    b2r[pl.ds(b, 1)] = tile2[None]

    def spread(k, carry):
        send(b2s, b2r.at[b], b2_ss, b2_rs, (seq_peer(k), r))
        return carry

    lax.fori_loop(0, N_SEQ - 1, spread, 0)

    wait_bytes(xr.at[pl.ds(0, 7)], x_rs)
    eye2 = where(iota((64, 128), 1) % 64 == iota((64, 128), 0), 1.0, 0.0).astype(BF16)
    half = iota((64, 128), 1) < 64
    xT = []
    for u in range(4):
        rows_u = xr[:, u].astype(F32).reshape(64, 128)
        both = jnp.concatenate([where(half, rows_u, 0.0), where(half, 0.0, rows_u)], axis=0)
        xT.append(mm_nt(eye2, both.astype(BF16)))
    xT = jnp.concatenate(xT, axis=1)
    nT = norm_rows(xT, 0).astype(BF16)
    proj = mm(winT, nT)
    qT = (proj[0:64] * (1.0 / math.sqrt(8))).astype(BF16).astype(F32)
    kT = proj[64:128].astype(BF16)
    vT = proj[128:192].astype(BF16)
    gate = jax.nn.sigmoid(proj[192:256])

    wait_bytes(w1r.at[pl.ds(0, 7)], w1_rs)
    w2 = jnp.sum(w1r[...], axis=0)
    w2s[...] = w2
    mine2 = bx * NC + bc
    w2r[pl.ds(mine2, 1)] = w2[None]
    for k in range(1, NX * NC):
        px = (bx + k // NC) % NX
        pc = (bc + k % NC) % NC
        send(w2s, w2r.at[mine2], w2_ss, w2_rs, (px * (NZ * NC) + bz * NC + pc, r))

    wait_bytes(b2r.at[pl.ds(0, N_SEQ - 1)], b2_rs)
    for hp in range(4):
        v = b2r[:, hp, :] + key_mask
        v2 = pltpu.roll(v, 64, 1)
        bias2[:, pl.ds(hp * 128, 128)] = where(half, v, v2)
        bias2[:, pl.ds((hp + 4) * 128, 128)] = where(half, v2, v)

    half2 = iota((64, 256), 1) % 128 < 64
    rowblk = iota((64, 128), 0) // 8
    gated = []
    for u in range(4):
        lanes = slice(u * 128, (u + 1) * 128)
        k_rows = kT[:, lanes].T
        q_u = qT[:, lanes]
        ctx = []
        for h in range(0, 8, 2):
            q2 = jnp.concatenate(
                [where(rowblk == h, q_u, 0.0), where(rowblk == h + 1, q_u, 0.0)], axis=1
            ).astype(BF16)
            sc = mm(k_rows, q2)
            sc = where(half2, sc[0:64], sc[64:128]) + bias2[:, pl.ds(h * 128, 256)]
            ex = jnp.exp(sc - jnp.max(sc, axis=0, keepdims=True))
            pb = ex * (1.0 / jnp.sum(ex, axis=0, keepdims=True))
            p2 = jnp.concatenate([where(half2, pb, 0.0), where(half2, 0.0, pb)], axis=0)
            cx = mm(vT[h * 8 : h * 8 + 16, lanes], p2.astype(BF16))
            ctx.append(cx[0:8, 0:128])
            ctx.append(cx[8:16, 128:256])
        gated.append((gate[:, lanes] * jnp.concatenate(ctx, axis=0)).astype(BF16))
    gT = jnp.concatenate(gated, axis=1)
    uT = mm(woutT, gT).astype(BF16).astype(F32)
    slot_lane = iota((1, 512), 1) // 64
    use_lane = jnp.zeros((1, 512), F32)
    for s in range(8):
        use_lane = where(slot_lane == s, use[s], use_lane)
    oT = norm_rows(xT + uT * use_lane, 0).astype(BF16)

    lane_s = iota((64, 256), 1) % 8
    left = jnp.zeros((64, 256), F32)
    right = jnp.zeros((128, 128), F32)
    lane_u2 = iota((128, 128), 1) // 32
    for u in range(4):
        o_rows = oT[:, u * 128 : (u + 1) * 128].T
        zl = mm(o_rows, wl)
        left = where(lane_s == 2 * u, zl[0:64], where(lane_s == 2 * u + 1, zl[64:128], left))
        right = where(lane_u2 == u, mm(o_rows, wr), right)
    right = right * scale_r
    for p in range(8):
        for sp in range(2):
            rs[p, sp] = right[sp * 64 + p * 8 : sp * 64 + p * 8 + 8].astype(BF16)
    rr[pl.ds(r, 1)] = rs[pl.ds(r, 1)]
    for k in far_first:
        p = res_peer(k)
        send(rs.at[p], rr.at[r], r_ss, r_rs, (b, p))
    left = (left * keep).astype(BF16)
    ls[...] = left
    lr[pl.ds(r, 1)] = left[None]
    for k in far_first:
        send(ls, lr.at[r], l_ss, l_rs, (b, res_peer(k)))

    for u in range(4):
        g_rows = gT[:, u * 128 : (u + 1) * 128].T
        z = mm(g_rows, wout2)
        on = where(half, use[2 * u], use[2 * u + 1])
        rows_u = where(half, z[0:64], z[64:128]).astype(BF16).astype(F32) * on
        us[:, u] = rows_u.reshape(8, 8, 128).astype(BF16)
    ur[pl.ds(r, 1)] = us[pl.ds(r, 1)]
    for k in far_first:
        p = res_peer(k)
        send(us.at[p], ur.at[r], u_ss, u_rs, (b, p))

    wait_bytes(rr.at[pl.ds(0, 7)], r_rs)
    packed = rr[...].astype(F32).reshape(128, 128).astype(BF16)
    ro = iota((512, 128), 0)
    co = iota((512, 128), 1)
    same = (ro // 64 == co // 16) & (ro % 2 == (co // 8) % 2) & ((ro // 8) % 8 == co % 8)
    spread_rows = mm(where(same, 1.0, 0.0).astype(BF16), packed)
    right_all = where((ro // 2) % 4 == co // 32, spread_rows, 0.0).astype(BF16)

    def times_weight(g, carry):
        t = mm(right_all, w4[g])
        for src in range(8):
            for j in range(8):
                a = src * 64 + j * 8
                v = jnp.concatenate([t[a : a + 8, 0:128], t[a : a + 8, 128:256]], axis=0)
                tt[j // 2, src, g, :, pl.ds((j % 2) * 128, 128)] = v.astype(BF16)
        return carry

    lax.fori_loop(0, 16, times_weight, 0)

    wait_bytes(lr.at[pl.ds(0, 7)], l_rs)
    for jp in range(4):
        acc = jnp.zeros((64, 256), F32)
        for src in range(8):
            acc = acc + mm(lr[src], tt[jp, src].reshape(256, 256))
        rows[pl.ds(2 * jp, 64, stride=8), :] = acc[:, 0:128]
        rows[pl.ds(2 * jp + 1, 64, stride=8), :] = acc[:, 128:256]
    ps[...] = rows[...].reshape(64, 8, 128).astype(BF16)
    pr[pl.ds(b, 1)] = ps[pl.ds(b, 1)]

    def scatter(k, carry):
        p = seq_peer(k)
        send(ps.at[p], pr.at[b], p_ss, p_rs, (p, r))
        return carry

    lax.fori_loop(0, N_SEQ - 1, scatter, 0)

    wait_bytes(ur.at[pl.ds(0, 7)], u_rs)
    back = ur[...].astype(F32).reshape(256, 128).astype(BF16)
    for sp in range(2):
        pick = where(iota((128, 64), 0) == iota((128, 64), 1) + 64 * sp, 1.0, 0.0).astype(BF16)
        upd_ref[:, sp] = mm(back, pick).reshape(32, 8, 64).astype(BF16)
    wait_bytes(w2r.at[pl.ds(0, 7)], w2_rs)
    weight_sum = jnp.sum(w2r[...], axis=0)

    wait_bytes(pr.at[pl.ds(0, N_SEQ - 1)], p_rs)
    summed = jnp.sum(pr[...].astype(F32), axis=0)
    pair_ref[...] = (summed / weight_sum + ob_ref[...]).astype(BF16)

    wait_bytes(xr.at[pl.ds(0, 7)], x_ss)
    wait_bytes(br.at[pl.ds(0, 7)], b_ss)
    wait_bytes(b2r.at[pl.ds(0, N_SEQ - 1)], b2_ss)
    wait_bytes(lr.at[pl.ds(0, 7)], l_ss)
    wait_bytes(rr.at[pl.ds(0, 7)], r_ss)
    wait_bytes(ur.at[pl.ds(0, 7)], u_ss)
    wait_bytes(pr.at[pl.ds(0, N_SEQ - 1)], p_ss)
    wait_bytes(w1r.at[pl.ds(0, 7)], w1_ss)
    wait_bytes(w2r.at[pl.ds(0, 7)], w2_ss)


def local(
    alignment_rows, pair_features, sequence_block_count, cluster_member_count,
    residue_present_mask, attention_in_weight, attention_out_weight, pair_bias_weight,
    outer_factor_weight, outer_output_weight, outer_product_bias,
):
    vm = pl.BlockSpec(memory_space=pltpu.VMEM)
    sm = pl.BlockSpec(memory_space=pltpu.SMEM)
    V = pltpu.VMEM
    update, pair = pl.pallas_call(
        kernel,
        out_shape=(
            jax.ShapeDtypeStruct((32, 2, 8, 64), BF16),
            jax.ShapeDtypeStruct((8, 128), BF16),
        ),
        in_specs=[vm, vm, sm, sm, vm, vm, vm, vm, vm, vm, vm],
        out_specs=(vm, vm),
        scratch_shapes=[
            V((8, 4, 8, 128), BF16), V((8, 4, 8, 128), BF16),
            V((4, 128), F32), V((8, 4, 128), F32),
            V((4, 128), F32), V((64, 4, 128), F32),
            V((64, 256), BF16), V((8, 64, 256), BF16),
            V((8, 2, 8, 128), BF16), V((8, 2, 8, 128), BF16),
            V((8, 4, 8, 128), BF16), V((8, 4, 8, 128), BF16),
            V((64, 8, 128), BF16), V((64, 8, 128), BF16),
            V((8, 128), F32), V((8, 8, 128), F32),
            V((8, 128), F32), V((8, 8, 128), F32),
            V((4, 8, 16, 16, 256), BF16), V((16, 128, 256), BF16),
            V((64, 1024), F32), V((512, 128), F32),
        ]
        + [pltpu.SemaphoreType.DMA] * 18,
        compiler_params=pltpu.CompilerParams(collective_id=0, has_side_effects=True),
    )(
        alignment_rows,
        pair_features.reshape(8, 128),
        sequence_block_count,
        cluster_member_count,
        residue_present_mask.reshape(1, 64),
        attention_in_weight,
        attention_out_weight,
        pair_bias_weight,
        outer_factor_weight,
        outer_output_weight,
        outer_product_bias.reshape(1, 128),
    )
    return update.reshape(64, 8, 64), pair.reshape(1, 8, 128)


def solution(mesh):
    return jax.shard_map(
        local,
        mesh=mesh,
        in_specs=(
            P("seq", "res", None), P("res", "seq", None), P("seq"), P("seq"),
            P(), P(), P(), P(), P(), P(), P(),
        ),
        out_specs=(P("seq", "res", None), P("seq", "res", None)),
        check_vma=False,
    )
```

```python
import functools
import math

import jax
import jax.numpy as jnp
from jax import lax
from jax.experimental import pallas as pl
from jax.experimental.pallas import tpu as pltpu
from jax.sharding import PartitionSpec as P

F32 = jnp.float32
BF16 = jnp.bfloat16
MESH = pl.DeviceIdType.MESH
HI = lax.Precision.HIGHEST
N_SEQ, N_RES = 64, 8
NX, NZ, NC = 4, 8, 2


def iota(shape, dim):
    return lax.broadcasted_iota(jnp.int32, shape, dim)


def where(cond, a, b):
    return jnp.where(cond, a, b)


def mm(a, b):
    return jnp.dot(a, b, preferred_element_type=F32)


def mm_nt(a, b, precision=None):
    dims = (((1,), (1,)), ((), ()))
    return lax.dot_general(a, b, dims, precision=precision, preferred_element_type=F32)


def mm_tn(a, b):
    return mm(a.T, b)


def norm_rows(v, axis):
    centre = jnp.mean(v, axis=axis, keepdims=True)
    spread = jnp.mean(jnp.square(v - centre), axis=axis, keepdims=True)
    return (v - centre) * lax.rsqrt(spread + 1e-05)


def wait_bytes(ref, sem):
    pltpu.make_async_copy(ref, ref, sem).wait()


def kernel(
    x_hbm, pf_hbm, cnt_ref, cmc_hbm, mask_hbm, win_hbm, wout_hbm, wb_hbm, wf_hbm, ow_hbm, ob_hbm,
    upd_ref, pair_ref,
    x_ref, pf_ref, cmc_ref, mask_ref, win_ref, wout_ref, wb_ref, wf_ref, ow_ref, ob_ref,
    xs, xr, bs, br, b2s, b2r, ls, lr, rs, rr, us, ur, ps, pr, w1s, w1r, w2s, w2r,
    tt, w4, bias2, rows, score, sums,
    in_sems,
    x_ss, x_rs, b_ss, b_rs, b2_ss, b2_rs, l_ss, l_rs, r_ss, r_rs, u_ss, u_rs, p_ss, p_rs,
    w1_ss, w1_rs, w2_ss, w2_rs, ready,
):
    b = lax.axis_index("seq")
    r = lax.axis_index("res")
    bx = b // (NZ * NC)
    bz = (b // NC) % NZ
    bc = b % NC

    px = [((bx + k) % NX) * (NZ * NC) for k in range(NX)]
    pz = [((bz + k) % NZ) * NC for k in range(NZ)]
    pc = [(bc + k) % NC for k in range(NC)]
    seq_peers = [
        px[kx] + pz[kz] + pc[kc]
        for kx in (2, 1, 3, 0)
        for kz in (4, 3, 5, 2, 6, 1, 7, 0)
        for kc in (1, 0)
        if kx + kz + kc > 0
    ]
    far_first = (4, 3, 5, 2, 6, 1, 7)
    res_peers = [(r + k) % N_RES for k in far_first]

    barrier = pltpu.get_barrier_semaphore()

    pairs_in = (
        (pf_hbm, pf_ref), (wb_hbm, wb_ref), (x_hbm, x_ref), (cmc_hbm, cmc_ref),
        (mask_hbm, mask_ref), (win_hbm, win_ref), (wout_hbm, wout_ref), (wf_hbm, wf_ref),
        (ow_hbm, ow_ref), (ob_hbm, ob_ref),
    )
    copies = [pltpu.make_async_copy(h, v, in_sems.at[n]) for n, (h, v) in enumerate(pairs_in)]

    def signal(sem, dev):
        pl.semaphore_signal(sem, inc=1, device_id=dev, device_id_type=MESH)

    z_peers = [px[0] + pz[k] + pc[0] for k in far_first]
    xc_peers = [px[k // NC] + pz[0] + pc[k % NC] for k in (4, 5, 2, 3, 6, 7, 1)]
    copies[0].start()
    copies[1].start()
    for p in z_peers:
        signal(barrier, (p, r))
    for p in res_peers:
        signal(barrier, (b, p))
    for p in xc_peers:
        signal(barrier, (p, r))
    for c in copies[2:]:
        c.start()
    copies[0].wait()
    copies[1].wait()

    pn = norm_rows(pf_ref[...].astype(F32), -1)
    pn = jnp.concatenate([pn] * 16, axis=0)
    pn = where((iota((128, 128), 0) // 8) % 8 == r, pn, 0.0)
    full = mm_nt(wb_ref[...], pn, HI)
    low = iota((4, 128), 1) < 64
    tile = where(low, full[0:4], full[4:8])
    bs[...] = tile
    br[pl.ds(r, 1)] = tile[None]

    pl.semaphore_wait(barrier, 21)
    for p in z_peers:
        signal(ready, (p, r))

    def send(src, dst, ss, rsem, dev):
        pltpu.make_async_remote_copy(
            src_ref=src, dst_ref=dst, send_sem=ss, recv_sem=rsem, device_id=dev, device_id_type=MESH
        ).start()

    for p in res_peers:
        send(bs, br.at[r], b_ss, b_rs, (b, p))

    copies[2].wait()
    flat = x_ref[...].astype(F32).reshape(512, 64).astype(BF16)
    dup = where(iota((64, 128), 1) % 64 == iota((64, 128), 0), 1.0, 0.0).astype(BF16)
    wide = mm(flat, dup).reshape(32, 2, 8, 128)
    pairs = where(iota((32, 8, 128), 2) < 64, wide[:, 0], wide[:, 1])
    xs[...] = pairs.reshape(8, 4, 8, 128).astype(BF16)
    xr[pl.ds(r, 1)] = xs[pl.ds(r, 1)]

    for p in res_peers:
        send(xs.at[p], xr.at[r], x_ss, x_rs, (b, p))

    for c in copies[3:]:
        c.wait()
    count = cnt_ref[0]
    total = jnp.float32(0.0)
    for s in range(64):
        total = total + where(s < count, cmc_ref[s], 0).astype(F32)
    w1s[...] = jnp.full((8, 128), 1.0, F32) * total
    w1r[pl.ds(bz, 1)] = w1s[...][None]
    use = []
    weight = []
    for s in range(8):
        slot = r * 8 + s
        on = where(slot < count, 1.0, 0.0)
        use.append(on)
        weight.append(cmc_ref[slot].astype(F32) * on)

    row = jnp.broadcast_to(mask_ref[...].astype(F32), (64, 64))
    keep = jnp.sum(where(iota((64, 64), 0) == iota((64, 64), 1), row, 0.0), axis=1, keepdims=True)
    key_mask = where(keep == 1.0, 0.0, -1000000.0)

    lane_u = iota((64, 128), 1) // 32
    parts = []
    for sp in range(2):
        part = jnp.zeros((64, 128), F32)
        for u in range(4):
            part = where(lane_u == u, weight[2 * u + sp], part)
        parts.append(part * keep)
    scale_r = jnp.concatenate(parts, axis=0)

    for p in z_peers:
        send(w1s, w1r.at[bz], w1_ss, w1_rs, (p, r))

    wait_bytes(br.at[pl.ds(0, 7)], b_rs)
    tile2 = jnp.sum(br[...], axis=0)
    b2s[...] = tile2
    b2r[pl.ds(b, 1)] = tile2[None]

    pl.semaphore_wait(ready, 7)
    for p in seq_peers:
        send(b2s, b2r.at[b], b2_ss, b2_rs, (p, r))

    winT = win_ref[...].astype(F32).T.astype(BF16)
    woutT = wout_ref[...].astype(F32).T.astype(BF16)
    wout2 = mm(wout_ref[...], dup).astype(BF16)
    e_left = where(iota((64, 256), 0) == iota((64, 256), 1) // 8, 1.0, 0.0).astype(BF16)
    e_right = where(iota((64, 128), 0) == 32 + iota((64, 128), 1) % 32, 1.0, 0.0).astype(BF16)
    wl = mm(wf_ref[...], e_left).astype(BF16)
    wr = mm(wf_ref[...], e_right).astype(BF16)
    for c in range(32):
        block = ow_ref[pl.ds(c * 32, 32), :].astype(BF16)
        for q in range(4):
            w4[c // 2, pl.ds(q * 32, 32), pl.ds((c % 2) * 128, 128)] = block

    wait_bytes(xr.at[pl.ds(0, 7)], x_rs)
    eye2 = where(iota((64, 128), 1) % 64 == iota((64, 128), 0), 1.0, 0.0).astype(BF16)
    half = iota((64, 128), 1) < 64
    xT = []
    for u in range(4):
        rows_u = xr[:, u].astype(F32).reshape(64, 128)
        both = jnp.concatenate([where(half, rows_u, 0.0), where(half, 0.0, rows_u)], axis=0)
        xT.append(mm_nt(eye2, both.astype(BF16)))
    xT = jnp.concatenate(xT, axis=1)
    nT = norm_rows(xT, 0).astype(BF16)
    proj = mm(winT, nT)
    qT = (proj[0:64] * (1.0 / math.sqrt(8))).astype(BF16).astype(F32)
    kT = proj[64:128].astype(BF16)
    vT = proj[128:192].astype(BF16)
    gate = jax.nn.sigmoid(proj[192:256])

    half2 = iota((64, 256), 1) % 128 < 64
    rowblk = iota((64, 128), 0) // 8
    for u in range(4):
        lanes = slice(u * 128, (u + 1) * 128)
        k_rows = kT[:, lanes].T
        q_u = qT[:, lanes]
        for h in range(0, 8, 2):
            q2 = jnp.concatenate(
                [where(rowblk == h, q_u, 0.0), where(rowblk == h + 1, q_u, 0.0)], axis=1
            ).astype(BF16)
            sc = mm(k_rows, q2)
            score[u, :, pl.ds(h * 128, 256)] = where(half2, sc[0:64], sc[64:128])

    wait_bytes(w1r.at[pl.ds(0, 7)], w1_rs)
    w2 = jnp.sum(w1r[...], axis=0)
    w2s[...] = w2
    mine2 = bx * NC + bc
    w2r[pl.ds(mine2, 1)] = w2[None]
    for p in xc_peers:
        send(w2s, w2r.at[mine2], w2_ss, w2_rs, (p, r))

    wait_bytes(b2r.at[pl.ds(0, N_SEQ - 1)], b2_rs)
    for hp in range(4):
        v = b2r[:, hp, :] + key_mask
        v2 = pltpu.roll(v, 64, 1)
        bias2[:, pl.ds(hp * 128, 128)] = where(half, v, v2)
        bias2[:, pl.ds((hp + 4) * 128, 128)] = where(half, v2, v)

    gated = []
    for u in range(4):
        lanes = slice(u * 128, (u + 1) * 128)
        ctx = []
        for h in range(0, 8, 2):
            sc = score[u, :, pl.ds(h * 128, 256)] + bias2[:, pl.ds(h * 128, 256)]
            ex = jnp.exp(sc - jnp.max(sc, axis=0, keepdims=True))
            pb = ex * (1.0 / jnp.sum(ex, axis=0, keepdims=True))
            p2 = jnp.concatenate([where(half2, pb, 0.0), where(half2, 0.0, pb)], axis=0)
            cx = mm(vT[h * 8 : h * 8 + 16, lanes], p2.astype(BF16))
            ctx.append(cx[0:8, 0:128])
            ctx.append(cx[8:16, 128:256])
        gated.append((gate[:, lanes] * jnp.concatenate(ctx, axis=0)).astype(BF16))
    gT = jnp.concatenate(gated, axis=1)
    uT = mm(woutT, gT).astype(BF16).astype(F32)
    slot_lane = iota((1, 512), 1) // 64
    use_lane = jnp.zeros((1, 512), F32)
    for s in range(8):
        use_lane = where(slot_lane == s, use[s], use_lane)
    oT = norm_rows(xT + uT * use_lane, 0).astype(BF16)

    lane_s = iota((64, 256), 1) % 8
    left = jnp.zeros((64, 256), F32)
    right = jnp.zeros((128, 128), F32)
    lane_u2 = iota((128, 128), 1) // 32
    for u in range(4):
        o_rows = oT[:, u * 128 : (u + 1) * 128].T
        zl = mm(o_rows, wl)
        left = where(lane_s == 2 * u, zl[0:64], where(lane_s == 2 * u + 1, zl[64:128], left))
        right = where(lane_u2 == u, mm(o_rows, wr), right)
    right = right * scale_r
    for p in range(8):
        for sp in range(2):
            rs[p, sp] = right[sp * 64 + p * 8 : sp * 64 + p * 8 + 8].astype(BF16)
    rr[pl.ds(r, 1)] = rs[pl.ds(r, 1)]
    for p in res_peers:
        send(rs.at[p], rr.at[r], r_ss, r_rs, (b, p))
    left = (left * keep).astype(BF16)
    ls[...] = left
    lr[pl.ds(r, 1)] = left[None]
    near = (3, 5, 2, 6, 1, 7)
    for n, k in enumerate(near):
        send(ls, lr.at[r], l_ss, l_rs.at[n], (b, (r + k) % N_RES))

    for u in range(4):
        g_rows = gT[:, u * 128 : (u + 1) * 128].T
        z = mm(g_rows, wout2)
        on = where(half, use[2 * u], use[2 * u + 1])
        rows_u = where(half, z[0:64], z[64:128]).astype(BF16).astype(F32) * on
        us[:, u] = rows_u.reshape(8, 8, 128).astype(BF16)
    ur[pl.ds(r, 1)] = us[pl.ds(r, 1)]
    wait_bytes(rr.at[pl.ds(0, 7)], r_rs)
    packed = rr[...].astype(F32).reshape(128, 128).astype(BF16)
    ro = iota((512, 128), 0)
    co = iota((512, 128), 1)
    same = (ro // 64 == co // 16) & (ro % 2 == (co // 8) % 2) & ((ro // 8) % 8 == co % 8)
    spread_rows = mm(where(same, 1.0, 0.0).astype(BF16), packed)
    right_all = where((ro // 2) % 4 == co // 32, spread_rows, 0.0).astype(BF16)

    def times_weight(g, carry):
        t = mm(right_all, w4[g])
        for src in range(8):
            for j in range(8):
                a = src * 64 + j * 8
                v = jnp.concatenate([t[a : a + 8, 0:128], t[a : a + 8, 128:256]], axis=0)
                tt[j // 2, src, g, :, pl.ds((j % 2) * 128, 128)] = v.astype(BF16)
        return carry

    lax.fori_loop(0, 8, times_weight, 0, unroll=4)

    before = (r + 5) % N_RES
    after = (r + 3) % N_RES
    wait_bytes(lr.at[0], l_rs.at[0])
    part = lr.at[before, pl.ds(0, 32)]
    send(part, part, l_ss, l_rs.at[6], (b, (r + 1) % N_RES))
    wait_bytes(lr.at[0], l_rs.at[1])
    part = lr.at[after, pl.ds(32, 32)]
    send(part, part, l_ss, l_rs.at[7], (b, (r + 7) % N_RES))
    for p in res_peers:
        send(us.at[p], ur.at[r], u_ss, u_rs, (b, p))
    lax.fori_loop(8, 16, times_weight, 0, unroll=4)

    for n in range(2, 6):
        wait_bytes(lr.at[0], l_rs.at[n])
    for jp in range(4):
        acc = jnp.zeros((64, 256), F32)
        for k in (0, 1, 7, 2, 6, 3, 5):
            src = (r + k) % N_RES
            acc = acc + mm(lr[src], tt[jp, src].reshape(256, 256))
        sums[jp] = acc
    wait_bytes(lr.at[0, pl.ds(0, 32)], l_rs.at[6])
    wait_bytes(lr.at[0, pl.ds(0, 32)], l_rs.at[7])
    last = (r + 4) % N_RES
    for jp in range(4):
        acc = sums[jp] + mm(lr[last], tt[jp, last].reshape(256, 256))
        rows[pl.ds(2 * jp, 64, stride=8), :] = acc[:, 0:128]
        rows[pl.ds(2 * jp + 1, 64, stride=8), :] = acc[:, 128:256]
    ps[...] = rows[...].reshape(64, 8, 128).astype(BF16)
    pr[pl.ds(b, 1)] = ps[pl.ds(b, 1)]

    for p in seq_peers:
        send(ps.at[p], pr.at[b], p_ss, p_rs, (p, r))

    wait_bytes(ur.at[pl.ds(0, 7)], u_rs)
    back = ur[...].astype(F32).reshape(256, 128).astype(BF16)
    for sp in range(2):
        pick = where(iota((128, 64), 0) == iota((128, 64), 1) + 64 * sp, 1.0, 0.0).astype(BF16)
        upd_ref[:, sp] = mm(back, pick).reshape(32, 8, 64).astype(BF16)
    wait_bytes(w2r.at[pl.ds(0, 7)], w2_rs)
    weight_sum = jnp.sum(w2r[...], axis=0)

    wait_bytes(pr.at[pl.ds(0, N_SEQ - 1)], p_rs)
    summed = jnp.sum(pr[...].astype(F32), axis=0)
    pair_ref[...] = (summed / weight_sum + ob_ref[...]).astype(BF16)

    wait_bytes(xr.at[pl.ds(0, 7)], x_ss)
    wait_bytes(br.at[pl.ds(0, 7)], b_ss)
    wait_bytes(b2r.at[pl.ds(0, N_SEQ - 1)], b2_ss)
    wait_bytes(lr.at[pl.ds(0, 7)], l_ss)
    wait_bytes(rr.at[pl.ds(0, 7)], r_ss)
    wait_bytes(ur.at[pl.ds(0, 7)], u_ss)
    wait_bytes(pr.at[pl.ds(0, N_SEQ - 1)], p_ss)
    wait_bytes(w1r.at[pl.ds(0, 7)], w1_ss)
    wait_bytes(w2r.at[pl.ds(0, 7)], w2_ss)


def local(
    alignment_rows, pair_features, sequence_block_count, cluster_member_count,
    residue_present_mask, attention_in_weight, attention_out_weight, pair_bias_weight,
    outer_factor_weight, outer_output_weight, outer_product_bias,
):
    vm = pl.BlockSpec(memory_space=pltpu.VMEM)
    hbm = pl.BlockSpec(memory_space=pl.ANY)
    sm = pl.BlockSpec(memory_space=pltpu.SMEM)
    V = pltpu.VMEM
    update, pair = pl.pallas_call(
        kernel,
        out_shape=(
            V((32, 2, 8, 64), BF16),
            V((8, 128), BF16),
        ),
        in_specs=[hbm, hbm, sm] + [hbm] * 8,
        out_specs=(vm, vm),
        scratch_shapes=[
            V((64, 8, 64), BF16), V((8, 128), BF16), pltpu.SMEM((64,), jnp.int32),
            V((1, 64), jnp.int32), V((64, 256), BF16), V((64, 64), BF16), V((8, 128), F32),
            V((64, 64), BF16), V((1024, 128), F32), V((1, 128), F32),
            V((8, 4, 8, 128), BF16), V((8, 4, 8, 128), BF16),
            V((4, 128), F32), V((8, 4, 128), F32),
            V((4, 128), F32), V((64, 4, 128), F32),
            V((64, 256), BF16), V((8, 64, 256), BF16),
            V((8, 2, 8, 128), BF16), V((8, 2, 8, 128), BF16),
            V((8, 4, 8, 128), BF16), V((8, 4, 8, 128), BF16),
            V((64, 8, 128), BF16), V((64, 8, 128), BF16),
            V((8, 128), F32), V((8, 8, 128), F32),
            V((8, 128), F32), V((8, 8, 128), F32),
            V((4, 8, 16, 16, 256), BF16), V((16, 128, 256), BF16),
            V((64, 1024), F32), V((512, 128), F32), V((4, 64, 1024), F32), V((4, 64, 256), F32),
            pltpu.SemaphoreType.DMA((10,)),
        ]
        + [pltpu.SemaphoreType.DMA((8,)) if n == 7 else pltpu.SemaphoreType.DMA for n in range(18)]
        + [pltpu.SemaphoreType.REGULAR],
        compiler_params=pltpu.CompilerParams(collective_id=0, has_side_effects=True),
    )(
        alignment_rows,
        pair_features.reshape(8, 128),
        sequence_block_count,
        cluster_member_count,
        residue_present_mask.reshape(1, 64),
        attention_in_weight,
        attention_out_weight,
        pair_bias_weight.T,
        outer_factor_weight,
        outer_output_weight,
        outer_product_bias.reshape(1, 128),
    )
    return update.reshape(64, 8, 64), pair.reshape(1, 8, 128)


def solution(mesh):
    return jax.shard_map(
        local,
        mesh=mesh,
        in_specs=(
            P("seq", "res", None), P("res", "seq", None), P("seq"), P("seq"),
            P(), P(), P(), P(), P(), P(), P(),
        ),
        out_specs=(P("seq", "res", None), P("seq", "res", None)),
        check_vma=False,
    )
```

```python
import functools
import math

import jax
import jax.numpy as jnp
from jax import lax
from jax.experimental import pallas as pl
from jax.experimental.pallas import tpu as pltpu
from jax.sharding import PartitionSpec as P

F32 = jnp.float32
BF16 = jnp.bfloat16
MESH = pl.DeviceIdType.MESH
HI = lax.Precision.HIGHEST
N_SEQ, N_RES = 64, 8
NX, NZ, NC = 4, 8, 2


def iota(shape, dim):
    return lax.broadcasted_iota(jnp.int32, shape, dim)


def where(cond, a, b):
    return jnp.where(cond, a, b)


def mm(a, b):
    return jnp.dot(a, b, preferred_element_type=F32)


def mm_nt(a, b, precision=None):
    dims = (((1,), (1,)), ((), ()))
    return lax.dot_general(a, b, dims, precision=precision, preferred_element_type=F32)


def mm_tn(a, b):
    return mm(a.T, b)


def norm_rows(v, axis):
    centre = jnp.mean(v, axis=axis, keepdims=True)
    spread = jnp.mean(jnp.square(v - centre), axis=axis, keepdims=True)
    return (v - centre) * lax.rsqrt(spread + 1e-05)


def wait_bytes(ref, sem):
    pltpu.make_async_copy(ref, ref, sem).wait()


def kernel(
    x_hbm, pf_hbm, cnt_ref, cmc_hbm, mask_hbm, win_hbm, wout_hbm, wb_hbm, wf_hbm, ow_hbm, ob_hbm,
    upd_ref, pair_ref,
    x_ref, pf_ref, cmc_ref, mask_ref, win_ref, wout_ref, wb_ref, wf_ref, ow_ref, ob_ref,
    xs, xr, bs, br, b2s, b2r, ls, lr, rs, rr, us, ur, ps, pr, w1s, w1r, w2s, w2r,
    tt, w4, bias2, spare, score, sums,
    in_sems,
    x_ss, x_rs, b_ss, b_rs, b2_ss, b2_rs, l_ss, l_rs, r_ss, r_rs, u_ss, u_rs, p_ss, p_rs,
    w1_ss, w1_rs, w2_ss, w2_rs, ready,
):
    b = lax.axis_index("seq")
    r = lax.axis_index("res")
    bx = b // (NZ * NC)
    bz = (b // NC) % NZ
    bc = b % NC

    px = [((bx + k) % NX) * (NZ * NC) for k in range(NX)]
    pz = [((bz + k) % NZ) * NC for k in range(NZ)]
    pc = [(bc + k) % NC for k in range(NC)]
    seq_peers = [
        px[kx] + pz[kz] + pc[kc]
        for kx in (2, 1, 3, 0)
        for kz in (4, 3, 5, 2, 6, 1, 7, 0)
        for kc in (1, 0)
        if kx + kz + kc > 0
    ]
    far_first = (4, 3, 5, 2, 6, 1, 7)
    res_peers = [(r + k) % N_RES for k in far_first]

    barrier = pltpu.get_barrier_semaphore()

    pairs_in = (
        (pf_hbm, pf_ref), (wb_hbm, wb_ref), (x_hbm, x_ref), (cmc_hbm, cmc_ref),
        (mask_hbm, mask_ref), (win_hbm, win_ref), (wout_hbm, wout_ref), (wf_hbm, wf_ref),
        (ow_hbm, ow_ref), (ob_hbm, ob_ref),
    )
    copies = [pltpu.make_async_copy(h, v, in_sems.at[n]) for n, (h, v) in enumerate(pairs_in)]

    def signal(sem, dev):
        pl.semaphore_signal(sem, inc=1, device_id=dev, device_id_type=MESH)

    z_peers = [px[0] + pz[k] + pc[0] for k in far_first]
    xc = (4, 5, 2, 3, 6, 7, 1)
    xc_peers = [px[k // NC] + pz[0] + pc[k % NC] for k in xc]
    member = (bx % NX) * NC + bc

    def member_at(k):
        return ((bx + k // NC) % NX) * NC + (bc + k % NC) % NC

    def member_from(k):
        return ((bx + NX - k // NC) % NX) * NC + (bc + k % NC) % NC

    copies[0].start()
    copies[1].start()
    for p in z_peers:
        signal(barrier, (p, r))
    for p in res_peers:
        signal(barrier, (b, p))
    for p in xc_peers:
        signal(barrier, (p, r))
    for c in copies[2:]:
        c.start()
    copies[0].wait()
    copies[1].wait()

    pn = norm_rows(pf_ref[...].astype(F32), -1)
    pn = jnp.concatenate([pn] * 16, axis=0)
    pn = where((iota((128, 128), 0) // 8) % 8 == r, pn, 0.0)
    full = mm_nt(wb_ref[...], pn, HI)
    low = iota((4, 128), 1) < 64
    tile = where(low, full[0:4], full[4:8])
    bs[...] = tile
    br[pl.ds(r, 1)] = tile[None]

    pl.semaphore_wait(barrier, 21)
    for p in z_peers:
        signal(ready, (p, r))

    def send(src, dst, ss, rsem, dev):
        pltpu.make_async_remote_copy(
            src_ref=src, dst_ref=dst, send_sem=ss, recv_sem=rsem, device_id=dev, device_id_type=MESH
        ).start()

    for p in res_peers:
        send(bs, br.at[r], b_ss, b_rs, (b, p))

    copies[2].wait()
    flat = x_ref[...].astype(F32).reshape(512, 64).astype(BF16)
    dup = where(iota((64, 128), 1) % 64 == iota((64, 128), 0), 1.0, 0.0).astype(BF16)
    wide = mm(flat, dup).reshape(32, 2, 8, 128)
    pairs = where(iota((32, 8, 128), 2) < 64, wide[:, 0], wide[:, 1])
    xs[...] = pairs.reshape(8, 4, 8, 128).astype(BF16)
    xr[pl.ds(r, 1)] = xs[pl.ds(r, 1)]

    for p in res_peers:
        send(xs.at[p], xr.at[r], x_ss, x_rs, (b, p))

    for c in copies[3:]:
        c.wait()
    count = cnt_ref[0]
    total = jnp.float32(0.0)
    for s in range(64):
        total = total + where(s < count, cmc_ref[s], 0).astype(F32)
    w1s[...] = jnp.full((8, 128), 1.0, F32) * total
    w1r[pl.ds(bz, 1)] = w1s[...][None]
    use = []
    weight = []
    for s in range(8):
        slot = r * 8 + s
        on = where(slot < count, 1.0, 0.0)
        use.append(on)
        weight.append(cmc_ref[slot].astype(F32) * on)

    row = jnp.broadcast_to(mask_ref[...].astype(F32), (64, 64))
    keep = jnp.sum(where(iota((64, 64), 0) == iota((64, 64), 1), row, 0.0), axis=1, keepdims=True)
    key_mask = where(keep == 1.0, 0.0, -1000000.0)

    lane_s = iota((1, 256), 1) % 8
    weight_lane = jnp.zeros((1, 256), F32)
    for n in range(8):
        weight_lane = where(lane_s == n, weight[n], weight_lane)

    for p in z_peers:
        send(w1s, w1r.at[bz], w1_ss, w1_rs, (p, r))

    wait_bytes(br.at[pl.ds(0, 7)], b_rs)
    tile2 = jnp.sum(br[...], axis=0)
    b2s[...] = tile2
    b2r[pl.ds(b, 1)] = tile2[None]

    pl.semaphore_wait(ready, 7)
    for p in seq_peers:
        send(b2s, b2r.at[b], b2_ss, b2_rs, (p, r))

    winT = win_ref[...].astype(F32).T.astype(BF16)
    woutT = wout_ref[...].astype(F32).T.astype(BF16)
    wout2 = mm(wout_ref[...], dup).astype(BF16)
    e_left = where(iota((64, 128), 0) == iota((64, 128), 1) % 32, 1.0, 0.0).astype(BF16)
    e_right = where(iota((64, 256), 0) == 32 + iota((64, 256), 1) // 8, 1.0, 0.0).astype(BF16)
    wl = mm(wf_ref[...], e_left).astype(BF16)
    wr = mm(wf_ref[...], e_right).astype(BF16)
    for d in range(32):
        w4[d // 2, :, pl.ds((d % 2) * 128, 128)] = ow_ref[pl.ds(d, 32, stride=32), :].astype(BF16)

    wait_bytes(xr.at[pl.ds(0, 7)], x_rs)
    eye2 = where(iota((64, 128), 1) % 64 == iota((64, 128), 0), 1.0, 0.0).astype(BF16)
    half = iota((64, 128), 1) < 64
    xT = []
    for u in range(4):
        rows_u = xr[:, u].astype(F32).reshape(64, 128)
        both = jnp.concatenate([where(half, rows_u, 0.0), where(half, 0.0, rows_u)], axis=0)
        xT.append(mm_nt(eye2, both.astype(BF16)))
    xT = jnp.concatenate(xT, axis=1)
    nT = norm_rows(xT, 0).astype(BF16)
    proj = mm(winT, nT)
    qT = (proj[0:64] * (1.0 / math.sqrt(8))).astype(BF16).astype(F32)
    kT = proj[64:128].astype(BF16)
    vT = proj[128:192].astype(BF16)
    gate = jax.nn.sigmoid(proj[192:256])

    half2 = iota((64, 256), 1) % 128 < 64
    rowblk = iota((64, 128), 0) // 8
    for u in range(4):
        lanes = slice(u * 128, (u + 1) * 128)
        k_rows = kT[:, lanes].T
        q_u = qT[:, lanes]
        for h in range(0, 8, 2):
            q2 = jnp.concatenate(
                [where(rowblk == h, q_u, 0.0), where(rowblk == h + 1, q_u, 0.0)], axis=1
            ).astype(BF16)
            sc = mm(k_rows, q2)
            score[u, :, pl.ds(h * 128, 256)] = where(half2, sc[0:64], sc[64:128])

    wait_bytes(w1r.at[pl.ds(0, 7)], w1_rs)
    w2 = jnp.sum(w1r[...], axis=0)
    w2s[...] = w2
    mine2 = bx * NC + bc
    w2r[pl.ds(mine2, 1)] = w2[None]
    for p in xc_peers:
        send(w2s, w2r.at[mine2], w2_ss, w2_rs, (p, r))

    wait_bytes(b2r.at[pl.ds(0, N_SEQ - 1)], b2_rs)
    for hp in range(4):
        v = b2r[:, hp, :] + key_mask
        v2 = pltpu.roll(v, 64, 1)
        bias2[:, pl.ds(hp * 128, 128)] = where(half, v, v2)
        bias2[:, pl.ds((hp + 4) * 128, 128)] = where(half, v2, v)

    gated = []
    for u in range(4):
        lanes = slice(u * 128, (u + 1) * 128)
        ctx = []
        for h in range(0, 8, 2):
            sc = score[u, :, pl.ds(h * 128, 256)] + bias2[:, pl.ds(h * 128, 256)]
            ex = jnp.exp(sc - jnp.max(sc, axis=0, keepdims=True))
            pb = ex * (1.0 / jnp.sum(ex, axis=0, keepdims=True))
            p2 = jnp.concatenate([where(half2, pb, 0.0), where(half2, 0.0, pb)], axis=0)
            cx = mm(vT[h * 8 : h * 8 + 16, lanes], p2.astype(BF16))
            ctx.append(cx[0:8, 0:128])
            ctx.append(cx[8:16, 128:256])
        gated.append((gate[:, lanes] * jnp.concatenate(ctx, axis=0)).astype(BF16))
    gT = jnp.concatenate(gated, axis=1)
    uT = mm(woutT, gT).astype(BF16).astype(F32)
    slot_lane = iota((1, 512), 1) // 64
    use_lane = jnp.zeros((1, 512), F32)
    for s in range(8):
        use_lane = where(slot_lane == s, use[s], use_lane)
    oT = norm_rows(xT + uT * use_lane, 0).astype(BF16)

    lane_s = iota((64, 256), 1) % 8
    lane_u = iota((128, 128), 1) // 32
    right = jnp.zeros((64, 256), F32)
    left = jnp.zeros((128, 128), F32)
    for u in range(4):
        o_rows = oT[:, u * 128 : (u + 1) * 128].T
        zr = mm(o_rows, wr)
        right = where(lane_s == 2 * u, zr[0:64], where(lane_s == 2 * u + 1, zr[64:128], right))
        left = where(lane_u == u, mm(o_rows, wl), left)
    spare[...] = left * jnp.concatenate([keep, keep], axis=0)
    for q in range(8):
        for sp in range(2):
            first = sp * 64 + (q // NC) * (NZ * NC) + q % NC
            rs[q, sp] = spare[pl.ds(first, 8, stride=2), :].astype(BF16)
    rr[pl.ds(member, 1)] = rs[pl.ds(member, 1)]
    for n, p in enumerate(xc_peers):
        send(rs.at[member_at(xc[n])], rr.at[member], r_ss, r_rs.at[n], (p, r))
    right = (right * keep * weight_lane).astype(BF16)
    ls[...] = right
    lr[pl.ds(member, 1)] = right[None]
    for n, p in enumerate(xc_peers):
        send(ls, lr.at[member], l_ss, l_rs.at[n], (p, r))

    for u in range(4):
        g_rows = gT[:, u * 128 : (u + 1) * 128].T
        z = mm(g_rows, wout2)
        on = where(half, use[2 * u], use[2 * u + 1])
        rows_u = where(half, z[0:64], z[64:128]).astype(BF16).astype(F32) * on
        us[:, u] = rows_u.reshape(8, 8, 128).astype(BF16)
    ur[pl.ds(r, 1)] = us[pl.ds(r, 1)]
    for p in res_peers:
        send(us.at[p], ur.at[r], u_ss, u_rs, (b, p))
    fold = where(iota((128, 32), 0) % 32 == iota((128, 32), 1), 1.0, 0.0).astype(BF16)

    def times_weight(srcs):
        n = len(srcs)
        packed = jnp.concatenate([rr[q].astype(F32).reshape(16, 128) for q in srcs], axis=0)
        ro = iota((64 * n, 16 * n), 0)
        co = iota((64 * n, 16 * n), 1)
        same = (ro // 64 == co // 16) & (ro % 2 == (co // 8) % 2) & ((ro // 8) % 8 == co % 8)
        spread_rows = mm(where(same, 1.0, 0.0).astype(BF16), packed.astype(BF16))
        own = (iota((64 * n, 128), 0) // 2) % 4 == iota((64 * n, 128), 1) // 32
        left_n = mm(where(own, spread_rows, 0.0).astype(BF16), fold).astype(BF16)

        for g in range(16):
            t = mm(left_n, w4[g])
            for m, q in enumerate(srcs):
                for i in range(8):
                    a = m * 64 + i * 8
                    v = jnp.concatenate([t[a : a + 8, 0:128], t[a : a + 8, 128:256]], axis=0)
                    tt[i // 2, q, g, :, pl.ds((i % 2) * 128, 128)] = v.astype(BF16)

    def products(srcs, ip):
        acc = jnp.zeros((64, 256), F32)
        for src in srcs:
            acc = acc + mm(lr[src], tt[ip, src].reshape(256, 256))
        return acc

    early = [member, member_from(xc[6])]
    late = [member_from(k) for k in xc[:6]]
    wait_bytes(rr.at[0], r_rs.at[6])
    times_weight(early)
    wait_bytes(lr.at[0], l_rs.at[6])
    for ip in range(4):
        sums[ip] = products(early, ip)
    for n in range(6):
        wait_bytes(rr.at[0], r_rs.at[n])
    times_weight(late)
    for n in range(6):
        wait_bytes(lr.at[0], l_rs.at[n])
    for ip in range(4):
        acc = sums[ip] + products(late, ip)
        ps[pl.ds(16 * ip, 8)] = acc[:, 0:128].reshape(8, 8, 128).astype(BF16)
        ps[pl.ds(16 * ip + 8, 8)] = acc[:, 128:256].reshape(8, 8, 128).astype(BF16)
    place = bz * N_RES + r
    pr[pl.ds(place, 1)] = ps[pl.ds(place, 1)]
    for kz in far_first + (0,):
        for ky in far_first + (0,):
            if kz + ky > 0:
                qz = (bz + kz) % NZ
                qy = (r + ky) % N_RES
                dev = (px[0] + pz[kz] + pc[0], qy)
                send(ps.at[qz * N_RES + qy], pr.at[place], p_ss, p_rs, dev)

    wait_bytes(ur.at[pl.ds(0, 7)], u_rs)
    back = ur[...].astype(F32).reshape(256, 128).astype(BF16)
    for sp in range(2):
        pick = where(iota((128, 64), 0) == iota((128, 64), 1) + 64 * sp, 1.0, 0.0).astype(BF16)
        upd_ref[:, sp] = mm(back, pick).reshape(32, 8, 64).astype(BF16)
    wait_bytes(w2r.at[pl.ds(0, 7)], w2_rs)
    weight_sum = jnp.sum(w2r[...], axis=0)

    wait_bytes(pr.at[pl.ds(0, 63)], p_rs)
    summed = jnp.sum(pr[...].astype(F32), axis=0)
    pair_ref[...] = (summed / weight_sum + ob_ref[...]).astype(BF16)

    wait_bytes(xr.at[pl.ds(0, 7)], x_ss)
    wait_bytes(br.at[pl.ds(0, 7)], b_ss)
    wait_bytes(b2r.at[pl.ds(0, N_SEQ - 1)], b2_ss)
    wait_bytes(lr.at[pl.ds(0, 7)], l_ss)
    wait_bytes(rr.at[pl.ds(0, 7)], r_ss)
    wait_bytes(ur.at[pl.ds(0, 7)], u_ss)
    wait_bytes(pr.at[pl.ds(0, 63)], p_ss)
    wait_bytes(w1r.at[pl.ds(0, 7)], w1_ss)
    wait_bytes(w2r.at[pl.ds(0, 7)], w2_ss)


def put_kernel(upd_in, pair_in, upd_out, pair_out, sems):
    first = pltpu.make_async_copy(upd_in, upd_out, sems.at[0])
    second = pltpu.make_async_copy(pair_in, pair_out, sems.at[1])
    first.start()
    second.start()
    first.wait()
    second.wait()


def local(
    alignment_rows, pair_features, sequence_block_count, cluster_member_count,
    residue_present_mask, attention_in_weight, attention_out_weight, pair_bias_weight,
    outer_factor_weight, outer_output_weight, outer_product_bias,
):
    vm = pl.BlockSpec(memory_space=pltpu.VMEM)
    hbm = pl.BlockSpec(memory_space=pl.ANY)
    sm = pl.BlockSpec(memory_space=pltpu.SMEM)
    V = pltpu.VMEM
    update, pair = pl.pallas_call(
        kernel,
        out_shape=(
            V((32, 2, 8, 64), BF16),
            V((8, 128), BF16),
        ),
        in_specs=[hbm, hbm, sm] + [hbm] * 8,
        out_specs=(vm, vm),
        scratch_shapes=[
            V((64, 8, 64), BF16), V((8, 128), BF16), pltpu.SMEM((64,), jnp.int32),
            V((1, 64), jnp.int32), V((64, 256), BF16), V((64, 64), BF16), V((8, 128), F32),
            V((64, 64), BF16), V((1024, 128), F32), V((1, 128), F32),
            V((8, 4, 8, 128), BF16), V((8, 4, 8, 128), BF16),
            V((4, 128), F32), V((8, 4, 128), F32),
            V((4, 128), F32), V((64, 4, 128), F32),
            V((64, 256), BF16), V((8, 64, 256), BF16),
            V((8, 2, 8, 128), BF16), V((8, 2, 8, 128), BF16),
            V((8, 4, 8, 128), BF16), V((8, 4, 8, 128), BF16),
            V((64, 8, 128), BF16), V((64, 8, 128), BF16),
            V((8, 128), F32), V((8, 8, 128), F32),
            V((8, 128), F32), V((8, 8, 128), F32),
            V((4, 8, 16, 16, 256), BF16), V((16, 32, 256), BF16),
            V((64, 1024), F32), V((128, 128), F32), V((4, 64, 1024), F32), V((4, 64, 256), F32),
            pltpu.SemaphoreType.DMA((10,)),
        ]
        + [pltpu.SemaphoreType.DMA((8,)) if n in (7, 9) else pltpu.SemaphoreType.DMA for n in range(18)]
        + [pltpu.SemaphoreType.REGULAR],
        compiler_params=pltpu.CompilerParams(collective_id=0, has_side_effects=True),
    )(
        alignment_rows,
        pair_features.reshape(8, 128),
        sequence_block_count,
        cluster_member_count,
        residue_present_mask.reshape(1, 64),
        attention_in_weight,
        attention_out_weight,
        pair_bias_weight.T,
        outer_factor_weight,
        outer_output_weight,
        outer_product_bias.reshape(1, 128),
    )
    update, pair = pl.pallas_call(
        put_kernel,
        out_shape=(
            jax.ShapeDtypeStruct((64, 8, 64), BF16),
            jax.ShapeDtypeStruct((1, 8, 128), BF16),
        ),
        in_specs=[vm, vm],
        out_specs=(hbm, hbm),
        scratch_shapes=[pltpu.SemaphoreType.DMA((2,))],
    )(
        pltpu.with_memory_space_constraint(update.reshape(64, 8, 64), pltpu.VMEM),
        pltpu.with_memory_space_constraint(pair.reshape(1, 8, 128), pltpu.VMEM),
    )
    return update, pair


def solution(mesh):
    return jax.shard_map(
        local,
        mesh=mesh,
        in_specs=(
            P("seq", "res", None), P("res", "seq", None), P("seq"), P("seq"),
            P(), P(), P(), P(), P(), P(), P(),
        ),
        out_specs=(P("seq", "res", None), P("seq", "res", None)),
        check_vma=False,
    )
```

```python
import functools
import math

import jax
import jax.numpy as jnp
from jax import lax
from jax.experimental import pallas as pl
from jax.experimental.pallas import tpu as pltpu
from jax.sharding import PartitionSpec as P

F32 = jnp.float32
BF16 = jnp.bfloat16
MESH = pl.DeviceIdType.MESH
HI = lax.Precision.HIGHEST
N_SEQ, N_RES = 64, 8
NX, NZ, NC = 4, 8, 2


def iota(shape, dim):
    return lax.broadcasted_iota(jnp.int32, shape, dim)


def where(cond, a, b):
    return jnp.where(cond, a, b)


def mm(a, b):
    return jnp.dot(a, b, preferred_element_type=F32)


def mm_nt(a, b, precision=None):
    dims = (((1,), (1,)), ((), ()))
    return lax.dot_general(a, b, dims, precision=precision, preferred_element_type=F32)


def mm_tn(a, b):
    return mm(a.T, b)


def norm_rows(v, axis):
    centre = jnp.mean(v, axis=axis, keepdims=True)
    spread = jnp.mean(jnp.square(v - centre), axis=axis, keepdims=True)
    return (v - centre) * lax.rsqrt(spread + 1e-05)


def wait_bytes(ref, sem):
    pltpu.make_async_copy(ref, ref, sem).wait()


def kernel(
    x_hbm, pf_hbm, cnt_ref, cmc_hbm, mask_hbm, win_hbm, wout_hbm, wb_hbm, wf_hbm, ow_hbm, ob_hbm,
    upd_ref, pair_ref,
    x_ref, pf_ref, cmc_ref, mask_ref, win_ref, wout_ref, wb_ref, wf_ref, ow_ref, ob_ref,
    xs, xr, bs, br, b2s, b2r, ls, lr, rs, rr, us, ur, ps, pr, w1s, w1r, w2s, w2r,
    tt, w4, bias2, spare, gt, score, sums,
    in_sems,
    x_ss, x_rs, b_ss, b_rs, b2_ss, b2_rs, l_ss, l_rs, r_ss, r_rs, u_ss, u_rs, p_ss, p_rs,
    w1_ss, w1_rs, w2_ss, w2_rs, ready,
):
    b = lax.axis_index("seq")
    r = lax.axis_index("res")
    bx = b // (NZ * NC)
    bz = (b // NC) % NZ
    bc = b % NC

    px = [((bx + k) % NX) * (NZ * NC) for k in range(NX)]
    pz = [((bz + k) % NZ) * NC for k in range(NZ)]
    pc = [(bc + k) % NC for k in range(NC)]
    seq_peers = [
        px[kx] + pz[kz] + pc[kc]
        for kz in (4, 3, 5, 2, 6, 1, 7, 0)
        for kx in (2, 1, 3, 0)
        for kc in (1, 0)
        if kx + kz + kc > 0
    ]
    far_first = (4, 3, 5, 2, 6, 1, 7)
    res_peers = [(r + k) % N_RES for k in far_first]

    barrier = pltpu.get_barrier_semaphore()

    pairs_in = (
        (pf_hbm, pf_ref), (wb_hbm, wb_ref), (x_hbm, x_ref), (cmc_hbm, cmc_ref),
        (mask_hbm, mask_ref), (win_hbm, win_ref), (wout_hbm, wout_ref), (wf_hbm, wf_ref),
        (ow_hbm, ow_ref), (ob_hbm, ob_ref),
    )
    copies = [pltpu.make_async_copy(h, v, in_sems.at[n]) for n, (h, v) in enumerate(pairs_in)]

    def signal(sem, dev):
        pl.semaphore_signal(sem, inc=1, device_id=dev, device_id_type=MESH)

    z_peers = [px[0] + pz[k] + pc[0] for k in far_first]
    xc = (4, 5, 2, 3, 6, 7, 1)
    xc_peers = [px[k // NC] + pz[0] + pc[k % NC] for k in xc]
    member = (bx % NX) * NC + bc

    def member_at(k):
        return ((bx + k // NC) % NX) * NC + (bc + k % NC) % NC

    def member_from(k):
        return ((bx + NX - k // NC) % NX) * NC + (bc + k % NC) % NC

    copies[0].start()
    copies[1].start()
    for p in z_peers:
        signal(barrier, (p, r))
    for p in res_peers:
        signal(barrier, (b, p))
    for p in xc_peers:
        signal(barrier, (p, r))
    for c in copies[2:]:
        c.start()
    copies[0].wait()
    copies[1].wait()

    pn = norm_rows(pf_ref[...].astype(F32), -1)
    pn = jnp.concatenate([pn] * 16, axis=0)
    pn = where((iota((128, 128), 0) // 8) % 8 == r, pn, 0.0)
    full = mm_nt(wb_ref[...], pn, HI)
    low = iota((4, 128), 1) < 64
    tile = where(low, full[0:4], full[4:8])
    bs[...] = tile
    br[pl.ds(r, 1)] = tile[None]

    pl.semaphore_wait(barrier, 21)
    for p in z_peers:
        signal(ready, (p, r))

    def send(src, dst, ss, rsem, dev):
        pltpu.make_async_remote_copy(
            src_ref=src, dst_ref=dst, send_sem=ss, recv_sem=rsem, device_id=dev, device_id_type=MESH
        ).start()

    for p in res_peers:
        send(bs, br.at[r], b_ss, b_rs, (b, p))

    copies[2].wait()
    flat = x_ref[...].astype(F32).reshape(512, 64).astype(BF16)
    dup = where(iota((64, 128), 1) % 64 == iota((64, 128), 0), 1.0, 0.0).astype(BF16)
    wide = mm(flat, dup).reshape(32, 2, 8, 128)
    pairs = where(iota((32, 8, 128), 2) < 64, wide[:, 0], wide[:, 1])
    xs[...] = pairs.reshape(8, 4, 8, 128).astype(BF16)
    xr[pl.ds(r, 1)] = xs[pl.ds(r, 1)]

    for p in res_peers:
        send(xs.at[p], xr.at[r], x_ss, x_rs, (b, p))

    for c in copies[3:]:
        c.wait()
    count = cnt_ref[0]
    total = jnp.float32(0.0)
    for s in range(64):
        total = total + where(s < count, cmc_ref[s], 0).astype(F32)
    w1s[...] = jnp.full((8, 128), 1.0, F32) * total
    w1r[pl.ds(bz, 1)] = w1s[...][None]
    use = []
    weight = []
    for s in range(8):
        slot = r * 8 + s
        on = where(slot < count, 1.0, 0.0)
        use.append(on)
        weight.append(cmc_ref[slot].astype(F32) * on)

    row = jnp.broadcast_to(mask_ref[...].astype(F32), (64, 64))
    keep = jnp.sum(where(iota((64, 64), 0) == iota((64, 64), 1), row, 0.0), axis=1, keepdims=True)
    key_mask = where(keep == 1.0, 0.0, -1000000.0)

    lane_s = iota((1, 256), 1) % 8
    weight_lane = jnp.zeros((1, 256), F32)
    for n in range(8):
        weight_lane = where(lane_s == n, weight[n], weight_lane)

    for p in z_peers:
        send(w1s, w1r.at[bz], w1_ss, w1_rs, (p, r))

    wait_bytes(br.at[pl.ds(0, 7)], b_rs)
    tile2 = jnp.sum(br[...], axis=0)
    b2s[...] = tile2
    b2r[pl.ds(b, 1)] = tile2[None]

    pl.semaphore_wait(ready, 7)
    for p in seq_peers:
        send(b2s, b2r.at[b], b2_ss, b2_rs, (p, r))

    winT = win_ref[...].astype(F32).T.astype(BF16)
    woutT = wout_ref[...].astype(F32).T.astype(BF16)
    wout2 = mm(wout_ref[...], dup).astype(BF16)
    e_left = where(iota((64, 128), 0) == iota((64, 128), 1) % 32, 1.0, 0.0).astype(BF16)
    e_right = where(iota((64, 256), 0) == 32 + iota((64, 256), 1) // 8, 1.0, 0.0).astype(BF16)
    wl = mm(wf_ref[...], e_left).astype(BF16)
    wr = mm(wf_ref[...], e_right).astype(BF16)
    for d in range(32):
        block = ow_ref[pl.ds(d, 32, stride=32), :].astype(BF16)
        for q in range(4):
            w4[d // 2, pl.ds(q * 32, 32), pl.ds((d % 2) * 128, 128)] = block

    wait_bytes(xr.at[pl.ds(0, 7)], x_rs)
    eye2 = where(iota((64, 128), 1) % 64 == iota((64, 128), 0), 1.0, 0.0).astype(BF16)
    half = iota((64, 128), 1) < 64
    xT = []
    for u in range(4):
        rows_u = xr[:, u].astype(F32).reshape(64, 128)
        both = jnp.concatenate([where(half, rows_u, 0.0), where(half, 0.0, rows_u)], axis=0)
        xT.append(mm_nt(eye2, both.astype(BF16)))
    xT = jnp.concatenate(xT, axis=1)
    nT = norm_rows(xT, 0).astype(BF16)
    proj = mm(winT, nT)
    qT = (proj[0:64] * (1.0 / math.sqrt(8))).astype(BF16).astype(F32)
    kT = proj[64:128].astype(BF16)
    vT = proj[128:192].astype(BF16)
    gate = jax.nn.sigmoid(proj[192:256])

    half2 = iota((64, 256), 1) % 128 < 64
    rowblk = iota((64, 128), 0) // 8
    for u in range(4):
        lanes = slice(u * 128, (u + 1) * 128)
        k_rows = kT[:, lanes].T
        q_u = qT[:, lanes]
        for h in range(0, 8, 2):
            q2 = jnp.concatenate(
                [where(rowblk == h, q_u, 0.0), where(rowblk == h + 1, q_u, 0.0)], axis=1
            ).astype(BF16)
            sc = mm(k_rows, q2)
            score[u, :, pl.ds(h * 128, 256)] = where(half2, sc[0:64], sc[64:128])

    wait_bytes(w1r.at[pl.ds(0, 7)], w1_rs)
    w2 = jnp.sum(w1r[...], axis=0)
    w2s[...] = w2
    mine2 = bx * NC + bc
    w2r[pl.ds(mine2, 1)] = w2[None]
    for p in xc_peers:
        send(w2s, w2r.at[mine2], w2_ss, w2_rs, (p, r))

    wait_bytes(b2r.at[pl.ds(0, N_SEQ - 1)], b2_rs)
    for hp in range(4):
        v = b2r[:, hp, :] + key_mask
        v2 = pltpu.roll(v, 64, 1)
        bias2[:, pl.ds(hp * 128, 128)] = where(half, v, v2)
        bias2[:, pl.ds((hp + 4) * 128, 128)] = where(half, v2, v)

    gated = []
    for u in range(4):
        lanes = slice(u * 128, (u + 1) * 128)
        ctx = []
        for h in range(0, 8, 2):
            sc = score[u, :, pl.ds(h * 128, 256)] + bias2[:, pl.ds(h * 128, 256)]
            ex = jnp.exp(sc - jnp.max(sc, axis=0, keepdims=True))
            pb = ex * (1.0 / jnp.sum(ex, axis=0, keepdims=True))
            p2 = jnp.concatenate([where(half2, pb, 0.0), where(half2, 0.0, pb)], axis=0)
            cx = mm(vT[h * 8 : h * 8 + 16, lanes], p2.astype(BF16))
            ctx.append(cx[0:8, 0:128])
            ctx.append(cx[8:16, 128:256])
        gated.append((gate[:, lanes] * jnp.concatenate(ctx, axis=0)).astype(BF16))
    gT = jnp.concatenate(gated, axis=1)
    gt[...] = gT
    uT = mm(woutT, gT).astype(BF16).astype(F32)
    slot_lane = iota((1, 512), 1) // 64
    use_lane = jnp.zeros((1, 512), F32)
    for s in range(8):
        use_lane = where(slot_lane == s, use[s], use_lane)
    oT = norm_rows(xT + uT * use_lane, 0).astype(BF16)

    lane_s = iota((64, 256), 1) % 8
    lane_u = iota((128, 128), 1) // 32
    right = jnp.zeros((64, 256), F32)
    left = jnp.zeros((128, 128), F32)
    for u in range(4):
        o_rows = oT[:, u * 128 : (u + 1) * 128].T
        zr = mm(o_rows, wr)
        right = where(lane_s == 2 * u, zr[0:64], where(lane_s == 2 * u + 1, zr[64:128], right))
        left = where(lane_u == u, mm(o_rows, wl), left)
    spare[...] = left * jnp.concatenate([keep, keep], axis=0)
    for q in range(8):
        for sp in range(2):
            first = sp * 64 + (q // NC) * (NZ * NC) + q % NC
            rs[q, sp] = spare[pl.ds(first, 8, stride=2), :].astype(BF16)
    rr[pl.ds(member, 1)] = rs[pl.ds(member, 1)]
    for n, p in enumerate(xc_peers):
        send(rs.at[member_at(xc[n])], rr.at[member], r_ss, r_rs.at[n], (p, r))
    right = (right * keep * weight_lane).astype(BF16)
    ls[...] = right
    lr[pl.ds(member, 1)] = right[None]
    for n, p in enumerate(xc_peers):
        send(ls, lr.at[member], l_ss, l_rs.at[n], (p, r))

    def times_weight(srcs):
        n = len(srcs)
        packed = jnp.concatenate([rr[q].astype(F32).reshape(16, 128) for q in srcs], axis=0)
        ro = iota((64 * n, 16 * n), 0)
        co = iota((64 * n, 16 * n), 1)
        same = (ro // 64 == co // 16) & (ro % 2 == (co // 8) % 2) & ((ro // 8) % 8 == co % 8)
        spread_rows = mm(where(same, 1.0, 0.0).astype(BF16), packed.astype(BF16))
        own = (iota((64 * n, 128), 0) // 2) % 4 == iota((64 * n, 128), 1) // 32
        left_n = where(own, spread_rows, 0.0).astype(BF16)

        for g in range(16):
            t = mm(left_n, w4[g])
            for m, q in enumerate(srcs):
                for i in range(8):
                    a = m * 64 + i * 8
                    v = jnp.concatenate([t[a : a + 8, 0:128], t[a : a + 8, 128:256]], axis=0)
                    tt[i // 2, q, g, :, pl.ds((i % 2) * 128, 128)] = v.astype(BF16)

    def products(srcs, ip):
        acc = jnp.zeros((64, 256), F32)
        for src in srcs:
            acc = acc + mm(lr[src], tt[ip, src].reshape(256, 256))
        return acc

    early = [member, member_from(xc[6])]
    others = [member_from(k) for k in xc[2:6] + xc[:2]]
    wait_bytes(rr.at[0], r_rs.at[6])
    times_weight(early)
    wait_bytes(lr.at[0], l_rs.at[6])
    for ip in range(4):
        sums[ip] = products(early, ip)

    for u in range(4):
        g_rows = gt[:, pl.ds(u * 128, 128)].T
        z = mm(g_rows, wout2)
        on = where(half, use[2 * u], use[2 * u + 1])
        rows_u = where(half, z[0:64], z[64:128]).astype(BF16).astype(F32) * on
        us[:, u] = rows_u.reshape(8, 8, 128).astype(BF16)
    ur[pl.ds(r, 1)] = us[pl.ds(r, 1)]
    for p in res_peers:
        send(us.at[p], ur.at[r], u_ss, u_rs, (b, p))
    for n in (2, 3, 4, 5, 0, 1):
        wait_bytes(rr.at[0], r_rs.at[n])
    times_weight(others)
    for n in range(6):
        wait_bytes(lr.at[0], l_rs.at[n])
    place = bz * N_RES + r

    def finish(t):
        ip = (bz // 2 + t) % 4
        acc = sums[ip] + products(others, ip)
        for odd in range(2):
            part = acc[:, 128 * odd : 128 * odd + 128].reshape(8, 8, 128)
            ps[pl.ds((2 * ip + odd) * N_RES, 8)] = part.astype(BF16)

    def scatter(qz, ky):
        qy = (r + ky) % N_RES
        dev = (px[0] + qz * NC + pc[0], qy)
        send(ps.at[qz * N_RES + qy], pr.at[place], p_ss, p_rs, dev)

    finish(2)
    pair = 2 * ((bz // 2 + 2) % 4)
    for ky in far_first + (0,):
        for odd in range(2):
            scatter(pair + odd, ky)
    for t in (1, 3, 0):
        finish(t)
    pr[pl.ds(place, 1)] = ps[pl.ds(place, 1)]
    for ky in far_first + (0,):
        for t in (1, 3):
            pair = 2 * ((bz // 2 + t) % 4)
            for odd in range(2):
                scatter(pair + odd, ky)
        scatter(bz + 1 - 2 * (bz % 2), ky)
        if ky > 0:
            scatter(bz, ky)

    wait_bytes(ur.at[pl.ds(0, 7)], u_rs)
    back = ur[...].astype(F32).reshape(256, 128).astype(BF16)
    for sp in range(2):
        pick = where(iota((128, 64), 0) == iota((128, 64), 1) + 64 * sp, 1.0, 0.0).astype(BF16)
        upd_ref[:, sp] = mm(back, pick).reshape(32, 8, 64).astype(BF16)
    wait_bytes(w2r.at[pl.ds(0, 7)], w2_rs)
    weight_sum = jnp.sum(w2r[...], axis=0)

    wait_bytes(pr.at[pl.ds(0, 63)], p_rs)
    summed = jnp.sum(pr[...].astype(F32), axis=0)
    pair_ref[...] = (summed / weight_sum + ob_ref[...]).astype(BF16)

    wait_bytes(xr.at[pl.ds(0, 7)], x_ss)
    wait_bytes(br.at[pl.ds(0, 7)], b_ss)
    wait_bytes(b2r.at[pl.ds(0, N_SEQ - 1)], b2_ss)
    wait_bytes(lr.at[pl.ds(0, 7)], l_ss)
    wait_bytes(rr.at[pl.ds(0, 7)], r_ss)
    wait_bytes(ur.at[pl.ds(0, 7)], u_ss)
    wait_bytes(pr.at[pl.ds(0, 63)], p_ss)
    wait_bytes(w1r.at[pl.ds(0, 7)], w1_ss)
    wait_bytes(w2r.at[pl.ds(0, 7)], w2_ss)


def put_kernel(upd_in, pair_in, upd_out, pair_out, sems):
    first = pltpu.make_async_copy(upd_in, upd_out, sems.at[0])
    second = pltpu.make_async_copy(pair_in, pair_out, sems.at[1])
    first.start()
    second.start()
    first.wait()
    second.wait()


def local(
    alignment_rows, pair_features, sequence_block_count, cluster_member_count,
    residue_present_mask, attention_in_weight, attention_out_weight, pair_bias_weight,
    outer_factor_weight, outer_output_weight, outer_product_bias,
):
    vm = pl.BlockSpec(memory_space=pltpu.VMEM)
    hbm = pl.BlockSpec(memory_space=pl.ANY)
    sm = pl.BlockSpec(memory_space=pltpu.SMEM)
    V = pltpu.VMEM
    update, pair = pl.pallas_call(
        kernel,
        out_shape=(
            V((32, 2, 8, 64), BF16),
            V((8, 128), BF16),
        ),
        in_specs=[hbm, hbm, sm] + [hbm] * 8,
        out_specs=(vm, vm),
        scratch_shapes=[
            V((64, 8, 64), BF16), V((8, 128), BF16), pltpu.SMEM((64,), jnp.int32),
            V((1, 64), jnp.int32), V((64, 256), BF16), V((64, 64), BF16), V((8, 128), F32),
            V((64, 64), BF16), V((1024, 128), F32), V((1, 128), F32),
            V((8, 4, 8, 128), BF16), V((8, 4, 8, 128), BF16),
            V((4, 128), F32), V((8, 4, 128), F32),
            V((4, 128), F32), V((64, 4, 128), F32),
            V((64, 256), BF16), V((8, 64, 256), BF16),
            V((8, 2, 8, 128), BF16), V((8, 2, 8, 128), BF16),
            V((8, 4, 8, 128), BF16), V((8, 4, 8, 128), BF16),
            V((64, 8, 128), BF16), V((64, 8, 128), BF16),
            V((8, 128), F32), V((8, 8, 128), F32),
            V((8, 128), F32), V((8, 8, 128), F32),
            V((4, 8, 16, 16, 256), BF16), V((16, 128, 256), BF16),
            V((64, 1024), F32), V((128, 128), F32), V((64, 512), BF16), V((4, 64, 1024), F32), V((4, 64, 256), F32),
            pltpu.SemaphoreType.DMA((10,)),
        ]
        + [pltpu.SemaphoreType.DMA((8,)) if n in (7, 9) else pltpu.SemaphoreType.DMA for n in range(18)]
        + [pltpu.SemaphoreType.REGULAR],
        compiler_params=pltpu.CompilerParams(collective_id=0, has_side_effects=True),
    )(
        alignment_rows,
        pair_features.reshape(8, 128),
        sequence_block_count,
        cluster_member_count,
        residue_present_mask.reshape(1, 64),
        attention_in_weight,
        attention_out_weight,
        pair_bias_weight.T,
        outer_factor_weight,
        outer_output_weight,
        outer_product_bias.reshape(1, 128),
    )
    update, pair = pl.pallas_call(
        put_kernel,
        out_shape=(
            jax.ShapeDtypeStruct((64, 8, 64), BF16),
            jax.ShapeDtypeStruct((1, 8, 128), BF16),
        ),
        in_specs=[vm, vm],
        out_specs=(hbm, hbm),
        scratch_shapes=[pltpu.SemaphoreType.DMA((2,))],
    )(
        pltpu.with_memory_space_constraint(update.reshape(64, 8, 64), pltpu.VMEM),
        pltpu.with_memory_space_constraint(pair.reshape(1, 8, 128), pltpu.VMEM),
    )
    return update, pair


def solution(mesh):
    return jax.shard_map(
        local,
        mesh=mesh,
        in_specs=(
            P("seq", "res", None), P("res", "seq", None), P("seq"), P("seq"),
            P(), P(), P(), P(), P(), P(), P(),
        ),
        out_specs=(P("seq", "res", None), P("seq", "res", None)),
        check_vma=False,
    )
```

```python
import functools
import math

import jax
import jax.numpy as jnp
from jax import lax
from jax.experimental import pallas as pl
from jax.experimental.pallas import tpu as pltpu
from jax.sharding import PartitionSpec as P

F32 = jnp.float32
BF16 = jnp.bfloat16
MESH = pl.DeviceIdType.MESH
HI = lax.Precision.HIGHEST
N_SEQ, N_RES = 64, 8
NX, NZ, NC = 4, 8, 2


def iota(shape, dim):
    return lax.broadcasted_iota(jnp.int32, shape, dim)


def where(cond, a, b):
    return jnp.where(cond, a, b)


def mm(a, b):
    return jnp.dot(a, b, preferred_element_type=F32)


def mm_nt(a, b, precision=None):
    dims = (((1,), (1,)), ((), ()))
    return lax.dot_general(a, b, dims, precision=precision, preferred_element_type=F32)


def mm_tn(a, b):
    return mm(a.T, b)


def norm_rows(v, axis):
    centre = jnp.mean(v, axis=axis, keepdims=True)
    spread = jnp.mean(jnp.square(v - centre), axis=axis, keepdims=True)
    return (v - centre) * lax.rsqrt(spread + 1e-05)


def wait_bytes(ref, sem):
    pltpu.make_async_copy(ref, ref, sem).wait()


def kernel(
    x_hbm, pf_hbm, cnt_ref, cmc_hbm, mask_hbm, win_hbm, wout_hbm, wb_hbm, wf_hbm, ow_hbm, ob_hbm,
    upd_ref, pair_ref,
    x_ref, pf_ref, cmc_ref, mask_ref, win_ref, wout_ref, wb_ref, wf_ref, ow_ref, ob_ref,
    xs, xr, bs, br, b2s, b2r, ls, lr, rs, rr, us, ur, ps, pr, w1s, w1r, w2s, w2r,
    tt, w4, bias2, spare, gt, vv, score, sums,
    in_sems,
    x_ss, x_rs, b_ss, b_rs, b2_ss, b2_rs, l_ss, l_rs, r_ss, r_rs, u_ss, u_rs, p_ss, p_rs,
    w1_ss, w1_rs, w2_ss, w2_rs, ready,
):
    b = lax.axis_index("seq")
    r = lax.axis_index("res")
    bx = b // (NZ * NC)
    bz = (b // NC) % NZ
    bc = b % NC

    px = [((bx + k) % NX) * (NZ * NC) for k in range(NX)]
    pz = [((bz + k) % NZ) * NC for k in range(NZ)]
    pc = [(bc + k) % NC for k in range(NC)]
    seq_peers = [
        px[kx] + pz[kz] + pc[kc]
        for kz in (4, 3, 5, 2, 6, 1, 7, 0)
        for kx in (2, 1, 3, 0)
        for kc in (1, 0)
        if kx + kz + kc > 0
    ]
    far_first = (4, 3, 5, 2, 6, 1, 7)
    res_peers = [(r + k) % N_RES for k in far_first]

    barrier = pltpu.get_barrier_semaphore()

    pairs_in = (
        (pf_hbm, pf_ref), (wb_hbm, wb_ref), (x_hbm, x_ref), (cmc_hbm, cmc_ref),
        (mask_hbm, mask_ref), (win_hbm, win_ref), (wout_hbm, wout_ref), (wf_hbm, wf_ref),
        (ow_hbm, ow_ref), (ob_hbm, ob_ref),
    )
    copies = [pltpu.make_async_copy(h, v, in_sems.at[n]) for n, (h, v) in enumerate(pairs_in)]

    def signal(sem, dev):
        pl.semaphore_signal(sem, inc=1, device_id=dev, device_id_type=MESH)

    z_peers = [px[0] + pz[k] + pc[0] for k in far_first]
    xc = (4, 5, 2, 3, 6, 7, 1)
    xc_peers = [px[k // NC] + pz[0] + pc[k % NC] for k in xc]
    member = (bx % NX) * NC + bc

    def member_at(k):
        return ((bx + k // NC) % NX) * NC + (bc + k % NC) % NC

    def member_from(k):
        return ((bx + NX - k // NC) % NX) * NC + (bc + k % NC) % NC

    copies[0].start()
    copies[1].start()
    for p in z_peers:
        signal(barrier, (p, r))
    for p in res_peers:
        signal(barrier, (b, p))
    for p in xc_peers:
        signal(barrier, (p, r))
    for c in copies[2:]:
        c.start()
    copies[0].wait()
    copies[1].wait()

    pn = norm_rows(pf_ref[...].astype(F32), -1)
    pn = jnp.concatenate([pn] * 16, axis=0)
    pn = where((iota((128, 128), 0) // 8) % 8 == r, pn, 0.0)
    full = mm_nt(wb_ref[...], pn, HI)
    low = iota((4, 128), 1) < 64
    tile = where(low, full[0:4], full[4:8])
    bs[...] = tile
    br[pl.ds(r, 1)] = tile[None]

    pl.semaphore_wait(barrier, 21)
    def send(src, dst, ss, rsem, dev):
        pltpu.make_async_remote_copy(
            src_ref=src, dst_ref=dst, send_sem=ss, recv_sem=rsem, device_id=dev, device_id_type=MESH
        ).start()

    for p in res_peers:
        send(bs, br.at[r], b_ss, b_rs, (b, p))
    for p in z_peers:
        signal(ready, (p, r))

    copies[2].wait()
    flat = x_ref[...].astype(F32).reshape(512, 64).astype(BF16)
    dup = where(iota((64, 128), 1) % 64 == iota((64, 128), 0), 1.0, 0.0).astype(BF16)
    wide = mm(flat, dup).reshape(32, 2, 8, 128)
    pairs = where(iota((32, 8, 128), 2) < 64, wide[:, 0], wide[:, 1])
    xs[...] = pairs.reshape(8, 4, 8, 128).astype(BF16)
    xr[pl.ds(r, 1)] = xs[pl.ds(r, 1)]

    for p in res_peers:
        send(xs.at[p], xr.at[r], x_ss, x_rs, (b, p))

    for c in copies[3:]:
        c.wait()
    count = cnt_ref[0]
    total = jnp.float32(0.0)
    for s in range(64):
        total = total + where(s < count, cmc_ref[s], 0).astype(F32)
    w1s[...] = jnp.full((8, 128), 1.0, F32) * total
    w1r[pl.ds(bz, 1)] = w1s[...][None]
    use = []
    weight = []
    for s in range(8):
        slot = r * 8 + s
        on = where(slot < count, 1.0, 0.0)
        use.append(on)
        weight.append(cmc_ref[slot].astype(F32) * on)

    row = jnp.broadcast_to(mask_ref[...].astype(F32), (64, 64))
    keep = jnp.sum(where(iota((64, 64), 0) == iota((64, 64), 1), row, 0.0), axis=1, keepdims=True)
    key_mask = where(keep == 1.0, 0.0, -1000000.0)

    lane_s = iota((1, 256), 1) % 8
    weight_lane = jnp.zeros((1, 256), F32)
    for n in range(8):
        weight_lane = where(lane_s == n, weight[n], weight_lane)

    for p in z_peers:
        send(w1s, w1r.at[bz], w1_ss, w1_rs, (p, r))

    wait_bytes(br.at[pl.ds(0, 7)], b_rs)
    tile2 = jnp.sum(br[...], axis=0)
    b2s[...] = tile2
    b2r[pl.ds(b, 1)] = tile2[None]

    pl.semaphore_wait(ready, 7)
    for p in seq_peers:
        send(b2s, b2r.at[b], b2_ss, b2_rs, (p, r))

    winT = win_ref[...].astype(F32).T.astype(BF16)
    woutT = wout_ref[...].astype(F32).T.astype(BF16)
    wout2 = mm(wout_ref[...], dup).astype(BF16)
    e_left = where(iota((64, 128), 0) == iota((64, 128), 1) % 32, 1.0, 0.0).astype(BF16)
    e_right = where(iota((64, 256), 0) == 32 + iota((64, 256), 1) // 8, 1.0, 0.0).astype(BF16)
    wl = mm(wf_ref[...], e_left).astype(BF16)
    wr = mm(wf_ref[...], e_right).astype(BF16)
    for d in range(32):
        block = ow_ref[pl.ds(d, 32, stride=32), :].astype(BF16)
        for q in range(4):
            w4[d // 2, pl.ds(q * 32, 32), pl.ds((d % 2) * 128, 128)] = block

    wait_bytes(xr.at[pl.ds(0, 7)], x_rs)
    eye2 = where(iota((64, 128), 1) % 64 == iota((64, 128), 0), 1.0, 0.0).astype(BF16)
    half = iota((64, 128), 1) < 64
    xT = []
    for u in range(4):
        rows_u = xr[:, u].astype(F32).reshape(64, 128)
        both = jnp.concatenate([where(half, rows_u, 0.0), where(half, 0.0, rows_u)], axis=0)
        xT.append(mm_nt(eye2, both.astype(BF16)))
    xT = jnp.concatenate(xT, axis=1)
    nT = norm_rows(xT, 0).astype(BF16)
    proj = mm(winT, nT)
    qT = (proj[0:64] * (1.0 / math.sqrt(8))).astype(BF16).astype(F32)
    kT = proj[64:128].astype(BF16)
    for u in range(4):
        for sp in range(2):
            first = u * 128 + sp * 64
            vv[u, pl.ds(sp * 64, 64), :] = proj[128:192, first : first + 64].astype(BF16)
    gate = jax.nn.sigmoid(proj[192:256])

    half2 = iota((64, 256), 1) % 128 < 64
    rowblk = iota((64, 128), 0) // 8
    for u in range(4):
        lanes = slice(u * 128, (u + 1) * 128)
        k_rows = kT[:, lanes].T
        q_u = qT[:, lanes]
        for h in range(0, 8, 2):
            q2 = jnp.concatenate(
                [where(rowblk == h, q_u, 0.0), where(rowblk == h + 1, q_u, 0.0)], axis=1
            ).astype(BF16)
            sc = mm(k_rows, q2)
            score[u, :, pl.ds(h * 128, 256)] = where(half2, sc[0:64], sc[64:128])

    wait_bytes(w1r.at[pl.ds(0, 7)], w1_rs)
    w2 = jnp.sum(w1r[...], axis=0)
    w2s[...] = w2
    mine2 = bx * NC + bc
    w2r[pl.ds(mine2, 1)] = w2[None]
    for p in xc_peers:
        send(w2s, w2r.at[mine2], w2_ss, w2_rs, (p, r))

    wait_bytes(b2r.at[pl.ds(0, N_SEQ - 1)], b2_rs)
    for hp in range(4):
        v = b2r[:, hp, :] + key_mask
        v2 = pltpu.roll(v, 64, 1)
        bias2[:, pl.ds(hp * 128, 128)] = where(half, v, v2)
        bias2[:, pl.ds((hp + 4) * 128, 128)] = where(half, v2, v)

    gated = []
    for u in range(4):
        lanes = slice(u * 128, (u + 1) * 128)
        ctx = []
        for h in range(0, 8, 2):
            sc = score[u, :, pl.ds(h * 128, 256)] + bias2[:, pl.ds(h * 128, 256)]
            ex = jnp.exp(sc - jnp.max(sc, axis=0, keepdims=True))
            pb = ex * (1.0 / jnp.sum(ex, axis=0, keepdims=True))
            v2 = jnp.concatenate(
                [vv[u, pl.ds(h * 8, 16), :], vv[u, pl.ds(64 + h * 8, 16), :]], axis=0
            )
            cx = mm(v2, pb.astype(BF16))
            cx = where(half2[0:16], cx[0:16], cx[16:32])
            ctx.append(cx[0:8, 0:128])
            ctx.append(cx[8:16, 128:256])
        gated.append((gate[:, lanes] * jnp.concatenate(ctx, axis=0)).astype(BF16))
    gT = jnp.concatenate(gated, axis=1)
    gt[...] = gT
    uT = mm(woutT, gT).astype(BF16).astype(F32)
    slot_lane = iota((1, 512), 1) // 64
    use_lane = jnp.zeros((1, 512), F32)
    for s in range(8):
        use_lane = where(slot_lane == s, use[s], use_lane)
    oT = norm_rows(xT + uT * use_lane, 0).astype(BF16)

    lane_s = iota((64, 256), 1) % 8
    lane_u = iota((128, 128), 1) // 32
    right = jnp.zeros((64, 256), F32)
    left = jnp.zeros((128, 128), F32)
    for u in range(4):
        o_rows = oT[:, u * 128 : (u + 1) * 128].T
        zr = mm(o_rows, wr)
        right = where(lane_s == 2 * u, zr[0:64], where(lane_s == 2 * u + 1, zr[64:128], right))
        left = where(lane_u == u, mm(o_rows, wl), left)
    spare[...] = left * jnp.concatenate([keep, keep], axis=0)
    for q in range(8):
        for sp in range(2):
            first = sp * 64 + (q // NC) * (NZ * NC) + q % NC
            rs[q, sp] = spare[pl.ds(first, 8, stride=2), :].astype(BF16)
    rr[pl.ds(member, 1)] = rs[pl.ds(member, 1)]
    for n, p in enumerate(xc_peers):
        send(rs.at[member_at(xc[n])], rr.at[member], r_ss, r_rs.at[n], (p, r))
    right = (right * keep * weight_lane).astype(BF16)
    ls[...] = right
    lr[pl.ds(member, 1)] = right[None]
    for n, p in enumerate(xc_peers):
        send(ls, lr.at[member], l_ss, l_rs.at[n], (p, r))

    def times_weight(srcs):
        n = len(srcs)
        packed = jnp.concatenate([rr[q].astype(F32).reshape(16, 128) for q in srcs], axis=0)
        ro = iota((64 * n, 16 * n), 0)
        co = iota((64 * n, 16 * n), 1)
        same = (ro // 64 == co // 16) & (ro % 2 == (co // 8) % 2) & ((ro // 8) % 8 == co % 8)
        spread_rows = mm(where(same, 1.0, 0.0).astype(BF16), packed.astype(BF16))
        own = (iota((64 * n, 128), 0) // 2) % 4 == iota((64 * n, 128), 1) // 32
        left_n = where(own, spread_rows, 0.0).astype(BF16)

        for g in range(16):
            t = mm(left_n, w4[g])
            for m, q in enumerate(srcs):
                for i in range(8):
                    a = m * 64 + i * 8
                    v = jnp.concatenate([t[a : a + 8, 0:128], t[a : a + 8, 128:256]], axis=0)
                    tt[i // 2, q, g, :, pl.ds((i % 2) * 128, 128)] = v.astype(BF16)

    def products(srcs, ip):
        acc = jnp.zeros((64, 256), F32)
        for src in srcs:
            acc = acc + mm(lr[src], tt[ip, src].reshape(256, 256))
        return acc

    early = [member, member_from(xc[6])]
    others = [member_from(k) for k in xc[2:6] + xc[:2]]
    wait_bytes(rr.at[0], r_rs.at[6])
    times_weight(early)
    wait_bytes(lr.at[0], l_rs.at[6])
    for ip in range(4):
        sums[ip] = products(early, ip)

    for u in range(4):
        g_rows = gt[:, pl.ds(u * 128, 128)].T
        z = mm(g_rows, wout2)
        on = where(half, use[2 * u], use[2 * u + 1])
        rows_u = where(half, z[0:64], z[64:128]).astype(BF16).astype(F32) * on
        us[:, u] = rows_u.reshape(8, 8, 128).astype(BF16)
    ur[pl.ds(r, 1)] = us[pl.ds(r, 1)]
    for p in res_peers:
        send(us.at[p], ur.at[r], u_ss, u_rs, (b, p))
    for n in (2, 3, 4, 5, 0, 1):
        wait_bytes(rr.at[0], r_rs.at[n])
    times_weight(others)
    for n in (4, 5, 0, 1):
        wait_bytes(lr.at[0], l_rs.at[n])
    for ip in range(4):
        sums[ip] = sums[ip] + products(others[2:], ip)
    for n in (2, 3):
        wait_bytes(lr.at[0], l_rs.at[n])
    place = bz * N_RES + r

    def finish(t):
        ip = (bz // 2 + t) % 4
        acc = sums[ip] + products(others[:2], ip)
        for odd in range(2):
            part = acc[:, 128 * odd : 128 * odd + 128].reshape(8, 8, 128)
            ps[pl.ds((2 * ip + odd) * N_RES, 8)] = part.astype(BF16)

    def scatter(qz, ky):
        qy = (r + ky) % N_RES
        dev = (px[0] + qz * NC + pc[0], qy)
        send(ps.at[qz * N_RES + qy], pr.at[place], p_ss, p_rs, dev)

    finish(2)
    pair = 2 * ((bz // 2 + 2) % 4)
    for ky in far_first + (0,):
        for odd in range(2):
            scatter(pair + odd, ky)
    for t in (1, 3, 0):
        finish(t)
    pr[pl.ds(place, 1)] = ps[pl.ds(place, 1)]
    for ky in far_first + (0,):
        for t in (1, 3):
            pair = 2 * ((bz // 2 + t) % 4)
            for odd in range(2):
                scatter(pair + odd, ky)
        scatter(bz + 1 - 2 * (bz % 2), ky)
        if ky > 0:
            scatter(bz, ky)

    wait_bytes(ur.at[pl.ds(0, 7)], u_rs)
    back = ur[...].astype(F32).reshape(256, 128).astype(BF16)
    for sp in range(2):
        pick = where(iota((128, 64), 0) == iota((128, 64), 1) + 64 * sp, 1.0, 0.0).astype(BF16)
        upd_ref[:, sp] = mm(back, pick).reshape(32, 8, 64).astype(BF16)
    wait_bytes(w2r.at[pl.ds(0, 7)], w2_rs)
    weight_sum = jnp.sum(w2r[...], axis=0)

    wait_bytes(pr.at[pl.ds(0, 63)], p_rs)
    summed = jnp.sum(pr[...].astype(F32), axis=0)
    pair_ref[...] = (summed / weight_sum + ob_ref[...]).astype(BF16)

    wait_bytes(xr.at[pl.ds(0, 7)], x_ss)
    wait_bytes(br.at[pl.ds(0, 7)], b_ss)
    wait_bytes(b2r.at[pl.ds(0, N_SEQ - 1)], b2_ss)
    wait_bytes(lr.at[pl.ds(0, 7)], l_ss)
    wait_bytes(rr.at[pl.ds(0, 7)], r_ss)
    wait_bytes(ur.at[pl.ds(0, 7)], u_ss)
    wait_bytes(pr.at[pl.ds(0, 63)], p_ss)
    wait_bytes(w1r.at[pl.ds(0, 7)], w1_ss)
    wait_bytes(w2r.at[pl.ds(0, 7)], w2_ss)


def put_kernel(upd_in, pair_in, upd_out, pair_out, sems):
    first = pltpu.make_async_copy(upd_in, upd_out, sems.at[0])
    second = pltpu.make_async_copy(pair_in, pair_out, sems.at[1])
    first.start()
    second.start()
    first.wait()
    second.wait()


def local(
    alignment_rows, pair_features, sequence_block_count, cluster_member_count,
    residue_present_mask, attention_in_weight, attention_out_weight, pair_bias_weight,
    outer_factor_weight, outer_output_weight, outer_product_bias,
):
    vm = pl.BlockSpec(memory_space=pltpu.VMEM)
    hbm = pl.BlockSpec(memory_space=pl.ANY)
    sm = pl.BlockSpec(memory_space=pltpu.SMEM)
    V = pltpu.VMEM
    update, pair = pl.pallas_call(
        kernel,
        out_shape=(
            V((32, 2, 8, 64), BF16),
            V((8, 128), BF16),
        ),
        in_specs=[hbm, hbm, sm] + [hbm] * 8,
        out_specs=(vm, vm),
        scratch_shapes=[
            V((64, 8, 64), BF16), V((8, 128), BF16), pltpu.SMEM((64,), jnp.int32),
            V((1, 64), jnp.int32), V((64, 256), BF16), V((64, 64), BF16), V((8, 128), F32),
            V((64, 64), BF16), V((1024, 128), F32), V((1, 128), F32),
            V((8, 4, 8, 128), BF16), V((8, 4, 8, 128), BF16),
            V((4, 128), F32), V((8, 4, 128), F32),
            V((4, 128), F32), V((64, 4, 128), F32),
            V((64, 256), BF16), V((8, 64, 256), BF16),
            V((8, 2, 8, 128), BF16), V((8, 2, 8, 128), BF16),
            V((8, 4, 8, 128), BF16), V((8, 4, 8, 128), BF16),
            V((64, 8, 128), BF16), V((64, 8, 128), BF16),
            V((8, 128), F32), V((8, 8, 128), F32),
            V((8, 128), F32), V((8, 8, 128), F32),
            V((4, 8, 16, 16, 256), BF16), V((16, 128, 256), BF16),
            V((64, 1024), F32), V((128, 128), F32), V((64, 512), BF16),
            V((4, 128, 64), BF16), V((4, 64, 1024), F32), V((4, 64, 256), F32),
            pltpu.SemaphoreType.DMA((10,)),
        ]
        + [pltpu.SemaphoreType.DMA((8,)) if n in (7, 9) else pltpu.SemaphoreType.DMA for n in range(18)]
        + [pltpu.SemaphoreType.REGULAR],
        compiler_params=pltpu.CompilerParams(collective_id=0, has_side_effects=True),
    )(
        alignment_rows,
        pair_features.reshape(8, 128),
        sequence_block_count,
        cluster_member_count,
        residue_present_mask.reshape(1, 64),
        attention_in_weight,
        attention_out_weight,
        pair_bias_weight.T,
        outer_factor_weight,
        outer_output_weight,
        outer_product_bias.reshape(1, 128),
    )
    update, pair = pl.pallas_call(
        put_kernel,
        out_shape=(
            jax.ShapeDtypeStruct((64, 8, 64), BF16),
            jax.ShapeDtypeStruct((1, 8, 128), BF16),
        ),
        in_specs=[vm, vm],
        out_specs=(hbm, hbm),
        scratch_shapes=[pltpu.SemaphoreType.DMA((2,))],
    )(
        pltpu.with_memory_space_constraint(update.reshape(64, 8, 64), pltpu.VMEM),
        pltpu.with_memory_space_constraint(pair.reshape(1, 8, 128), pltpu.VMEM),
    )
    return update, pair


def solution(mesh):
    return jax.shard_map(
        local,
        mesh=mesh,
        in_specs=(
            P("seq", "res", None), P("res", "seq", None), P("seq"), P("seq"),
            P(), P(), P(), P(), P(), P(), P(),
        ),
        out_specs=(P("seq", "res", None), P("seq", "res", None)),
        check_vma=False,
    )
```

```python
import functools
import math

import jax
import jax.numpy as jnp
from jax import lax
from jax.experimental import pallas as pl
from jax.experimental.pallas import tpu as pltpu
from jax.sharding import PartitionSpec as P

F32 = jnp.float32
BF16 = jnp.bfloat16
MESH = pl.DeviceIdType.MESH
HI = lax.Precision.HIGHEST
N_SEQ, N_RES = 64, 8
NX, NZ, NC = 4, 8, 2


def iota(shape, dim):
    return lax.broadcasted_iota(jnp.int32, shape, dim)


def where(cond, a, b):
    return jnp.where(cond, a, b)


def mm(a, b):
    return jnp.dot(a, b, preferred_element_type=F32)


def mm_nt(a, b, precision=None):
    dims = (((1,), (1,)), ((), ()))
    return lax.dot_general(a, b, dims, precision=precision, preferred_element_type=F32)


def mm_tn(a, b):
    return mm(a.T, b)


def norm_rows(v, axis):
    centre = jnp.mean(v, axis=axis, keepdims=True)
    spread = jnp.mean(jnp.square(v - centre), axis=axis, keepdims=True)
    return (v - centre) * lax.rsqrt(spread + 1e-05)


def wait_bytes(ref, sem):
    pltpu.make_async_copy(ref, ref, sem).wait()


def kernel(
    x_hbm, pf_hbm, cnt_ref, cmc_hbm, mask_hbm, win_hbm, wout_hbm, wb_hbm, wf_hbm, ow_hbm, ob_hbm,
    upd_ref, pair_ref,
    x_ref, pf_ref, cmc_ref, mask_ref, win_ref, wout_ref, wb_ref, wf_ref, ow_ref, ob_ref,
    xs, xr, bs, br, b2s, b2r, ls, lr, rs, rr, us, ur, ps, pr, w1s, w1r, w2s, w2r,
    tt, w4, bias2, spare, gt, vv, score, sums,
    in_sems,
    x_ss, x_rs, b_ss, b_rs, b2_ss, b2_rs, l_ss, l_rs, r_ss, r_rs, u_ss, u_rs, p_ss, p_rs,
    w1_ss, w1_rs, w2_ss, w2_rs, ready,
):
    b = lax.axis_index("seq")
    r = lax.axis_index("res")
    bx = b // (NZ * NC)
    bz = (b // NC) % NZ
    bc = b % NC

    px = [((bx + k) % NX) * (NZ * NC) for k in range(NX)]
    pz = [((bz + k) % NZ) * NC for k in range(NZ)]
    pc = [(bc + k) % NC for k in range(NC)]
    seq_peers = [
        px[kx] + pz[kz] + pc[kc]
        for kz in (4, 3, 5, 2, 6, 1, 7, 0)
        for kx in (2, 1, 3, 0)
        for kc in (1, 0)
        if kx + kz + kc > 0
    ]
    far_first = (4, 3, 5, 2, 6, 1, 7)
    res_peers = [(r + k) % N_RES for k in far_first]

    barrier = pltpu.get_barrier_semaphore()

    pairs_in = (
        (pf_hbm, pf_ref), (wb_hbm, wb_ref), (x_hbm, x_ref), (cmc_hbm, cmc_ref),
        (mask_hbm, mask_ref), (win_hbm, win_ref), (wout_hbm, wout_ref), (wf_hbm, wf_ref),
        (ow_hbm, ow_ref), (ob_hbm, ob_ref),
    )
    copies = [pltpu.make_async_copy(h, v, in_sems.at[n]) for n, (h, v) in enumerate(pairs_in)]

    def signal(sem, dev):
        pl.semaphore_signal(sem, inc=1, device_id=dev, device_id_type=MESH)

    z_peers = [px[0] + pz[k] + pc[0] for k in far_first]
    xc = (4, 5, 2, 3, 6, 7, 1)
    xc_peers = [px[k // NC] + pz[0] + pc[k % NC] for k in xc]
    member = (bx % NX) * NC + bc

    def member_at(k):
        return ((bx + k // NC) % NX) * NC + (bc + k % NC) % NC

    def member_from(k):
        return ((bx + NX - k // NC) % NX) * NC + (bc + k % NC) % NC

    copies[0].start()
    copies[1].start()
    for p in z_peers:
        signal(barrier, (p, r))
    for p in res_peers:
        signal(barrier, (b, p))
    for p in xc_peers:
        signal(barrier, (p, r))
    for c in copies[2:]:
        c.start()
    copies[0].wait()
    copies[1].wait()

    pn = norm_rows(pf_ref[...].astype(F32), -1)
    pn = jnp.concatenate([pn] * 16, axis=0)
    pn = where((iota((128, 128), 0) // 8) % 8 == r, pn, 0.0)
    full = mm_nt(wb_ref[...], pn, HI)
    low = iota((4, 128), 1) < 64
    tile = where(low, full[0:4], full[4:8])
    bs[...] = tile
    br[pl.ds(r, 1)] = tile[None]

    pl.semaphore_wait(barrier, 21)
    def send(src, dst, ss, rsem, dev):
        pltpu.make_async_remote_copy(
            src_ref=src, dst_ref=dst, send_sem=ss, recv_sem=rsem, device_id=dev, device_id_type=MESH
        ).start()

    for p in res_peers:
        send(bs, br.at[r], b_ss, b_rs, (b, p))
    for p in z_peers:
        signal(ready, (p, r))

    copies[2].wait()
    flat = x_ref[...].astype(F32).reshape(512, 64).astype(BF16)
    dup = where(iota((64, 128), 1) % 64 == iota((64, 128), 0), 1.0, 0.0).astype(BF16)
    wide = mm(flat, dup).reshape(32, 2, 8, 128)
    pairs = where(iota((32, 8, 128), 2) < 64, wide[:, 0], wide[:, 1])
    xs[...] = pairs.reshape(8, 4, 8, 128).astype(BF16)
    xr[pl.ds(r, 1)] = xs[pl.ds(r, 1)]

    for p in res_peers:
        send(xs.at[p], xr.at[r], x_ss, x_rs, (b, p))

    for c in copies[3:]:
        c.wait()
    count = cnt_ref[0]
    total = jnp.float32(0.0)
    for s in range(64):
        total = total + where(s < count, cmc_ref[s], 0).astype(F32)
    w1s[...] = jnp.full((8, 128), 1.0, F32) * total
    w1r[pl.ds(bz, 1)] = w1s[...][None]
    use = []
    weight = []
    for s in range(8):
        slot = r * 8 + s
        on = where(slot < count, 1.0, 0.0)
        use.append(on)
        weight.append(cmc_ref[slot].astype(F32) * on)

    row = jnp.broadcast_to(mask_ref[...].astype(F32), (64, 64))
    keep = jnp.sum(where(iota((64, 64), 0) == iota((64, 64), 1), row, 0.0), axis=1, keepdims=True)
    key_mask = where(keep == 1.0, 0.0, -1000000.0)

    lane_s = iota((1, 256), 1) % 8
    weight_lane = jnp.zeros((1, 256), F32)
    for n in range(8):
        weight_lane = where(lane_s == n, weight[n], weight_lane)

    for p in z_peers:
        send(w1s, w1r.at[bz], w1_ss, w1_rs, (p, r))

    wait_bytes(br.at[pl.ds(0, 7)], b_rs)
    tile2 = jnp.sum(br[...], axis=0)
    b2s[...] = tile2
    b2r[pl.ds(b, 1)] = tile2[None]

    pl.semaphore_wait(ready, 7)
    for p in seq_peers:
        send(b2s, b2r.at[b], b2_ss, b2_rs, (p, r))

    winT = win_ref[...].astype(F32).T.astype(BF16)
    woutT = wout_ref[...].astype(F32).T.astype(BF16)
    wout2 = mm(wout_ref[...], dup).astype(BF16)
    e_left = where(iota((64, 128), 0) == iota((64, 128), 1) % 32, 1.0, 0.0).astype(BF16)
    e_right = where(iota((64, 256), 0) == 32 + iota((64, 256), 1) // 8, 1.0, 0.0).astype(BF16)
    wl = mm(wf_ref[...], e_left).astype(BF16)
    wr = mm(wf_ref[...], e_right).astype(BF16)
    for d in range(32):
        block = ow_ref[pl.ds(d, 32, stride=32), :].astype(BF16)
        w4[d // 2, :, pl.ds((d % 2) * 128, 128)] = block

    wait_bytes(xr.at[pl.ds(0, 7)], x_rs)
    eye2 = where(iota((64, 128), 1) % 64 == iota((64, 128), 0), 1.0, 0.0).astype(BF16)
    half = iota((64, 128), 1) < 64
    xT = []
    for u in range(4):
        rows_u = xr[:, u].astype(F32).reshape(64, 128)
        both = jnp.concatenate([where(half, rows_u, 0.0), where(half, 0.0, rows_u)], axis=0)
        xT.append(mm_nt(eye2, both.astype(BF16)))
    xT = jnp.concatenate(xT, axis=1)
    nT = norm_rows(xT, 0).astype(BF16)
    proj = mm(winT, nT)
    qT = (proj[0:64] * (1.0 / math.sqrt(8))).astype(BF16).astype(F32)
    kT = proj[64:128].astype(BF16)
    for u in range(4):
        for sp in range(2):
            first = u * 128 + sp * 64
            vv[u, pl.ds(sp * 64, 64), :] = proj[128:192, first : first + 64].astype(BF16)
    gate = jax.nn.sigmoid(proj[192:256])

    half2 = iota((64, 256), 1) % 128 < 64
    rowblk = iota((64, 128), 0) // 8
    for u in range(4):
        lanes = slice(u * 128, (u + 1) * 128)
        k_rows = kT[:, lanes].T
        q_u = qT[:, lanes]
        for h in range(0, 8, 2):
            q2 = jnp.concatenate(
                [where(rowblk == h, q_u, 0.0), where(rowblk == h + 1, q_u, 0.0)], axis=1
            ).astype(BF16)
            sc = mm(k_rows, q2)
            score[u, :, pl.ds(h * 128, 256)] = where(half2, sc[0:64], sc[64:128])

    wait_bytes(w1r.at[pl.ds(0, 7)], w1_rs)
    w2 = jnp.sum(w1r[...], axis=0)
    w2s[...] = w2
    mine2 = bx * NC + bc
    w2r[pl.ds(mine2, 1)] = w2[None]
    for p in xc_peers:
        send(w2s, w2r.at[mine2], w2_ss, w2_rs, (p, r))

    wait_bytes(b2r.at[pl.ds(0, N_SEQ - 1)], b2_rs)
    for hp in range(4):
        v = b2r[:, hp, :] + key_mask
        v2 = pltpu.roll(v, 64, 1)
        bias2[:, pl.ds(hp * 128, 128)] = where(half, v, v2)
        bias2[:, pl.ds((hp + 4) * 128, 128)] = where(half, v2, v)

    gated = []
    for u in range(4):
        lanes = slice(u * 128, (u + 1) * 128)
        ctx = []
        for h in range(0, 8, 2):
            sc = score[u, :, pl.ds(h * 128, 256)] + bias2[:, pl.ds(h * 128, 256)]
            ex = jnp.exp(sc - jnp.max(sc, axis=0, keepdims=True))
            pb = ex * (1.0 / jnp.sum(ex, axis=0, keepdims=True))
            v2 = jnp.concatenate(
                [vv[u, pl.ds(h * 8, 16), :], vv[u, pl.ds(64 + h * 8, 16), :]], axis=0
            )
            cx = mm(v2, pb.astype(BF16))
            cx = where(half2[0:16], cx[0:16], cx[16:32])
            ctx.append(cx[0:8, 0:128])
            ctx.append(cx[8:16, 128:256])
        gated.append((gate[:, lanes] * jnp.concatenate(ctx, axis=0)).astype(BF16))
    gT = jnp.concatenate(gated, axis=1)
    gt[...] = gT
    uT = mm(woutT, gT).astype(BF16).astype(F32)
    slot_lane = iota((1, 512), 1) // 64
    use_lane = jnp.zeros((1, 512), F32)
    for s in range(8):
        use_lane = where(slot_lane == s, use[s], use_lane)
    oT = norm_rows(xT + uT * use_lane, 0).astype(BF16)

    lane_s = iota((64, 256), 1) % 8
    lane_u = iota((128, 128), 1) // 32
    right = jnp.zeros((64, 256), F32)
    left = jnp.zeros((128, 128), F32)
    for u in range(4):
        o_rows = oT[:, u * 128 : (u + 1) * 128].T
        zr = mm(o_rows, wr)
        right = where(lane_s == 2 * u, zr[0:64], where(lane_s == 2 * u + 1, zr[64:128], right))
        left = where(lane_u == u, mm(o_rows, wl), left)
    spare[...] = left * jnp.concatenate([keep, keep], axis=0)
    for q in range(8):
        for sp in range(2):
            first = sp * 64 + (q // NC) * (NZ * NC) + q % NC
            rs[q, sp] = spare[pl.ds(first, 8, stride=2), :].astype(BF16)
    rr[pl.ds(member, 1)] = rs[pl.ds(member, 1)]
    for n, p in enumerate(xc_peers):
        send(rs.at[member_at(xc[n])], rr.at[member], r_ss, r_rs.at[n], (p, r))
    right = (right * keep * weight_lane).astype(BF16)
    ls[...] = right
    lr[pl.ds(member, 1)] = right[None]
    for n, p in enumerate(xc_peers):
        send(ls, lr.at[member], l_ss, l_rs.at[n], (p, r))

    def times_weight(srcs):
        n = len(srcs)
        packed = jnp.concatenate([rr[q].astype(F32).reshape(16, 128) for q in srcs], axis=0)
        stack = jnp.concatenate([packed[:, u * 32 : u * 32 + 32] for u in range(4)], axis=0)
        ro = iota((64 * n, 64 * n), 0)
        co = iota((64 * n, 64 * n), 1)
        cu = co // (16 * n)
        cr = co % (16 * n)
        same = (ro // 64 == cr // 16) & (ro % 2 == (cr // 8) % 2) & ((ro // 8) % 8 == cr % 8)
        pick = where(same & ((ro // 2) % 4 == cu), 1.0, 0.0).astype(BF16)
        left_n = mm(pick, stack.astype(BF16)).astype(BF16)

        for g in range(16):
            t = mm(left_n, w4[g])
            for m, q in enumerate(srcs):
                for i in range(8):
                    a = m * 64 + i * 8
                    v = jnp.concatenate([t[a : a + 8, 0:128], t[a : a + 8, 128:256]], axis=0)
                    tt[i // 2, q, g, :, pl.ds((i % 2) * 128, 128)] = v.astype(BF16)

    def products(srcs, ip):
        acc = jnp.zeros((64, 256), F32)
        for src in srcs:
            acc = acc + mm(lr[src], tt[ip, src].reshape(256, 256))
        return acc

    early = [member, member_from(xc[6])]
    others = [member_from(k) for k in xc[2:6] + xc[:2]]
    wait_bytes(rr.at[0], r_rs.at[6])
    times_weight(early)
    wait_bytes(lr.at[0], l_rs.at[6])
    for ip in range(4):
        sums[ip] = products(early, ip)

    for u in range(4):
        g_rows = gt[:, pl.ds(u * 128, 128)].T
        z = mm(g_rows, wout2)
        on = where(half, use[2 * u], use[2 * u + 1])
        rows_u = where(half, z[0:64], z[64:128]).astype(BF16).astype(F32) * on
        us[:, u] = rows_u.reshape(8, 8, 128).astype(BF16)
    ur[pl.ds(r, 1)] = us[pl.ds(r, 1)]
    for p in res_peers:
        send(us.at[p], ur.at[r], u_ss, u_rs, (b, p))
    for n in (2, 3, 4, 5, 0, 1):
        wait_bytes(rr.at[0], r_rs.at[n])
    times_weight(others)
    for n in (4, 5, 0, 1):
        wait_bytes(lr.at[0], l_rs.at[n])
    for ip in range(4):
        sums[ip] = sums[ip] + products(others[2:], ip)
    for n in (2, 3):
        wait_bytes(lr.at[0], l_rs.at[n])
    place = bz * N_RES + r

    def finish(t):
        ip = (bz // 2 + t) % 4
        acc = sums[ip] + products(others[:2], ip)
        for odd in range(2):
            part = acc[:, 128 * odd : 128 * odd + 128].reshape(8, 8, 128)
            ps[pl.ds((2 * ip + odd) * N_RES, 8)] = part.astype(BF16)

    def scatter(qz, ky):
        qy = (r + ky) % N_RES
        dev = (px[0] + qz * NC + pc[0], qy)
        send(ps.at[qz * N_RES + qy], pr.at[place], p_ss, p_rs, dev)

    finish(2)
    pair = 2 * ((bz // 2 + 2) % 4)
    for ky in far_first + (0,):
        for odd in range(2):
            scatter(pair + odd, ky)
    for t in (1, 3, 0):
        finish(t)
    pr[pl.ds(place, 1)] = ps[pl.ds(place, 1)]
    for ky in far_first + (0,):
        for t in (1, 3):
            pair = 2 * ((bz // 2 + t) % 4)
            for odd in range(2):
                scatter(pair + odd, ky)
        scatter(bz + 1 - 2 * (bz % 2), ky)
        if ky > 0:
            scatter(bz, ky)

    wait_bytes(ur.at[pl.ds(0, 7)], u_rs)
    back = ur[...].astype(F32).reshape(256, 128).astype(BF16)
    for sp in range(2):
        pick = where(iota((128, 64), 0) == iota((128, 64), 1) + 64 * sp, 1.0, 0.0).astype(BF16)
        upd_ref[:, sp] = mm(back, pick).reshape(32, 8, 64).astype(BF16)
    wait_bytes(w2r.at[pl.ds(0, 7)], w2_rs)
    weight_sum = jnp.sum(w2r[...], axis=0)

    wait_bytes(pr.at[pl.ds(0, 63)], p_rs)
    summed = jnp.sum(pr[...].astype(F32), axis=0)
    pair_ref[...] = (summed / weight_sum + ob_ref[...]).astype(BF16)

    wait_bytes(xr.at[pl.ds(0, 7)], x_ss)
    wait_bytes(br.at[pl.ds(0, 7)], b_ss)
    wait_bytes(b2r.at[pl.ds(0, N_SEQ - 1)], b2_ss)
    wait_bytes(lr.at[pl.ds(0, 7)], l_ss)
    wait_bytes(rr.at[pl.ds(0, 7)], r_ss)
    wait_bytes(ur.at[pl.ds(0, 7)], u_ss)
    wait_bytes(pr.at[pl.ds(0, 63)], p_ss)
    wait_bytes(w1r.at[pl.ds(0, 7)], w1_ss)
    wait_bytes(w2r.at[pl.ds(0, 7)], w2_ss)


def put_kernel(upd_in, pair_in, upd_out, pair_out, sems):
    first = pltpu.make_async_copy(upd_in, upd_out, sems.at[0])
    second = pltpu.make_async_copy(pair_in, pair_out, sems.at[1])
    first.start()
    second.start()
    first.wait()
    second.wait()


def local(
    alignment_rows, pair_features, sequence_block_count, cluster_member_count,
    residue_present_mask, attention_in_weight, attention_out_weight, pair_bias_weight,
    outer_factor_weight, outer_output_weight, outer_product_bias,
):
    vm = pl.BlockSpec(memory_space=pltpu.VMEM)
    hbm = pl.BlockSpec(memory_space=pl.ANY)
    sm = pl.BlockSpec(memory_space=pltpu.SMEM)
    V = pltpu.VMEM
    update, pair = pl.pallas_call(
        kernel,
        out_shape=(
            V((32, 2, 8, 64), BF16),
            V((8, 128), BF16),
        ),
        in_specs=[hbm, hbm, sm] + [hbm] * 8,
        out_specs=(vm, vm),
        scratch_shapes=[
            V((64, 8, 64), BF16), V((8, 128), BF16), pltpu.SMEM((64,), jnp.int32),
            V((1, 64), jnp.int32), V((64, 256), BF16), V((64, 64), BF16), V((8, 128), F32),
            V((64, 64), BF16), V((1024, 128), F32), V((1, 128), F32),
            V((8, 4, 8, 128), BF16), V((8, 4, 8, 128), BF16),
            V((4, 128), F32), V((8, 4, 128), F32),
            V((4, 128), F32), V((64, 4, 128), F32),
            V((64, 256), BF16), V((8, 64, 256), BF16),
            V((8, 2, 8, 128), BF16), V((8, 2, 8, 128), BF16),
            V((8, 4, 8, 128), BF16), V((8, 4, 8, 128), BF16),
            V((64, 8, 128), BF16), V((64, 8, 128), BF16),
            V((8, 128), F32), V((8, 8, 128), F32),
            V((8, 128), F32), V((8, 8, 128), F32),
            V((4, 8, 16, 16, 256), BF16), V((16, 32, 256), BF16),
            V((64, 1024), F32), V((128, 128), F32), V((64, 512), BF16),
            V((4, 128, 64), BF16), V((4, 64, 1024), F32), V((4, 64, 256), F32),
            pltpu.SemaphoreType.DMA((10,)),
        ]
        + [pltpu.SemaphoreType.DMA((8,)) if n in (7, 9) else pltpu.SemaphoreType.DMA for n in range(18)]
        + [pltpu.SemaphoreType.REGULAR],
        compiler_params=pltpu.CompilerParams(collective_id=0, has_side_effects=True),
    )(
        alignment_rows,
        pair_features.reshape(8, 128),
        sequence_block_count,
        cluster_member_count,
        residue_present_mask.reshape(1, 64),
        attention_in_weight,
        attention_out_weight,
        pair_bias_weight.T,
        outer_factor_weight,
        outer_output_weight,
        outer_product_bias.reshape(1, 128),
    )
    update, pair = pl.pallas_call(
        put_kernel,
        out_shape=(
            jax.ShapeDtypeStruct((64, 8, 64), BF16),
            jax.ShapeDtypeStruct((1, 8, 128), BF16),
        ),
        in_specs=[vm, vm],
        out_specs=(hbm, hbm),
        scratch_shapes=[pltpu.SemaphoreType.DMA((2,))],
    )(
        pltpu.with_memory_space_constraint(update.reshape(64, 8, 64), pltpu.VMEM),
        pltpu.with_memory_space_constraint(pair.reshape(1, 8, 128), pltpu.VMEM),
    )
    return update, pair


def solution(mesh):
    return jax.shard_map(
        local,
        mesh=mesh,
        in_specs=(
            P("seq", "res", None), P("res", "seq", None), P("seq"), P("seq"),
            P(), P(), P(), P(), P(), P(), P(),
        ),
        out_specs=(P("seq", "res", None), P("seq", "res", None)),
        check_vma=False,
    )
```
